128 devices in a mesh: graph: 1, nodes: 128 (over z, y, x, core).
Axes of the slice: x: 4, y: 4, z: 4, core: 2. Of those that a mesh axis runs over, the one named last changes fastest.
Arguments:
- node_feats: bfloat16 [131072, 200], P(('graph', 'nodes'))
- a_int: bfloat16 [131072, 1024], P(('graph', 'nodes'))
- a_halo: bfloat16 [131072, 512], P(('graph', 'nodes'))
- send_idx: int32 [512, 128], P(('graph', 'nodes'))
- w_first: bfloat16 [200, 512], replicated
- w_second: bfloat16 [512, 107], replicated
- grad_out: bfloat16 [131072, 107], P(('graph', 'nodes'))
Outputs:
- output 1: float32 [200, 512], P('graph')
- output 2: float32 [512, 107], P('graph')
- output 3: float32 [131072, 200], P(('graph', 'nodes'))
All inputs are finite; a program needn't handle non-finite values.
Results may differ from the reference program's by a relative error of at most 0.00585534.
Values are sent between devices in bfloat16 or wider.
A program may use at most 1 GiB of HBM per device.

```python
import jax
import jax.numpy as jnp
from jax import lax

GROUP_SIZE = 128
NODES_DEV = 1024
HALO_SLOTS = 128
MAX_HOPS = 2
FEAT_IN = 200
HIDDEN = 512
CLASSES = 107
INNER_DEGREE = 16
HALO_DEGREE = 4

NUM_LINKS = 2 * MAX_HOPS
OFFSETS = [(link // 2 + 1) * (1 - 2 * (link % 2)) for link in range(NUM_LINKS)]


def draw_graph(key):
    key_count, key_order, key_blocks = jax.random.split(key, 3)
    window = 2 * HALO_SLOTS
    counts = jax.random.randint(key_count, (GROUP_SIZE, NUM_LINKS), HALO_SLOTS // 4, HALO_SLOTS + 1)
    counts = counts.at[0, 0].set(HALO_SLOTS)
    scores = jax.random.randint(key_order, (GROUP_SIZE, NUM_LINKS, window), 0, 65536) * window + jnp.arange(window)
    slot_order = jnp.argsort(scores, axis=-1)[:, :, :HALO_SLOTS]
    upward = jnp.array([offset > 0 for offset in OFFSETS])
    window_base = jnp.where(upward, NODES_DEV - window, 0)
    slot_pos = jnp.arange(HALO_SLOTS)
    used_slot = slot_pos[None, None, :] < counts[:, :, None]
    send_idx = jnp.where(used_slot, slot_order + window_base[None, :, None], 0).astype(jnp.int32)
    recv_counts = jnp.stack([jnp.roll(counts[:, link], OFFSETS[link]) for link in range(NUM_LINKS)], axis=1)
    row_pos = jnp.arange(NODES_DEV)
    low_half = row_pos < NODES_DEV // 2
    row_ok = jnp.where(upward[None, :], low_half[:, None], jnp.logical_not(low_half)[:, None])

    def one_device(inputs):
        dev_key, recv_count = inputs
        key_mask, key_inner, key_hmask, key_halo = jax.random.split(dev_key, 4)
        inner_mask = jnp.logical_or(jax.random.randint(key_mask, (NODES_DEV, NODES_DEV), 0, NODES_DEV) < INNER_DEGREE, row_pos[:, None] == row_pos[None, :])
        col_ok = slot_pos[None, :] < recv_count[:, None]
        halo_mask = (jax.random.randint(key_hmask, (NODES_DEV, NUM_LINKS, HALO_SLOTS), 0, HALO_SLOTS) < HALO_DEGREE) & row_ok[:, :, None] & col_ok[None, :, :]
        inner_w = jnp.where(inner_mask, jax.random.uniform(key_inner, (NODES_DEV, NODES_DEV), jnp.float32, 0.5, 1.5), 0.0)
        halo_w = jnp.where(halo_mask, jax.random.uniform(key_halo, (NODES_DEV, NUM_LINKS, HALO_SLOTS), jnp.float32, 0.5, 1.5), 0.0)
        degree = jnp.sum(inner_mask, axis=1) + jnp.sum(halo_mask, axis=(1, 2))
        row_scale = lax.rsqrt(degree.astype(jnp.float32))
        inner_adj = (inner_w * row_scale[:, None]).astype(jnp.bfloat16)
        halo_adj = (halo_w * row_scale[:, None, None]).reshape(NODES_DEV, NUM_LINKS * HALO_SLOTS).astype(jnp.bfloat16)
        return inner_adj, halo_adj

    inner_adj, halo_adj = lax.map(one_device, (jax.random.split(key_blocks, GROUP_SIZE), recv_counts))
    return (inner_adj.reshape(GROUP_SIZE * NODES_DEV, NODES_DEV), halo_adj.reshape(GROUP_SIZE * NODES_DEV, NUM_LINKS * HALO_SLOTS), send_idx.reshape(GROUP_SIZE * NUM_LINKS, HALO_SLOTS))


def setup_inputs(seed: int = 0, part: int = 0) -> dict:
    root_key = jax.random.key(seed)
    shared_key, parts_key = jax.random.split(root_key)
    key_first, key_second = jax.random.split(shared_key)
    part_key = jax.random.fold_in(parts_key, part)
    key_feats, key_grad, key_graph = jax.random.split(part_key, 3)
    rows_total = GROUP_SIZE * NODES_DEV
    node_feats = jax.random.normal(key_feats, (rows_total, FEAT_IN), jnp.float32).astype(jnp.bfloat16)
    grad_out = jax.random.normal(key_grad, (rows_total, CLASSES), jnp.float32).astype(jnp.bfloat16)
    w_first = (jax.random.normal(key_first, (FEAT_IN, HIDDEN), jnp.float32) * FEAT_IN ** -0.5).astype(jnp.bfloat16)
    w_second = (jax.random.normal(key_second, (HIDDEN, CLASSES), jnp.float32) * HIDDEN ** -0.5).astype(jnp.bfloat16)
    a_int, a_halo, send_idx = draw_graph(key_graph)
    return {"node_feats": node_feats, "a_int": a_int, "a_halo": a_halo, "send_idx": send_idx, "w_first": w_first, "w_second": w_second, "grad_out": grad_out}


def aggregate(a_int, a_halo, features, send_idx):
    feat_width = features.shape[-1]
    local_rows = features.reshape(GROUP_SIZE, NODES_DEV, feat_width)
    send_plan = send_idx.reshape(GROUP_SIZE, NUM_LINKS * HALO_SLOTS)
    sent_rows = jax.vmap(lambda rows_dev, plan_dev: jnp.take(rows_dev, plan_dev, axis=0))(local_rows, send_plan)
    sent_rows = sent_rows.reshape(GROUP_SIZE, NUM_LINKS, HALO_SLOTS, feat_width)
    halo_rows = jnp.stack([jnp.roll(sent_rows[:, link], OFFSETS[link], axis=0) for link in range(NUM_LINKS)], axis=1)
    halo_rows = halo_rows.reshape(GROUP_SIZE, NUM_LINKS * HALO_SLOTS, feat_width)
    blocks = (a_int.reshape(GROUP_SIZE, NODES_DEV, NODES_DEV), a_halo.reshape(GROUP_SIZE, NODES_DEV, NUM_LINKS * HALO_SLOTS), local_rows, halo_rows)

    def one_device(block):
        inner_adj, halo_adj, own_rows, remote_rows = block
        return jnp.dot(inner_adj, own_rows, preferred_element_type=jnp.float32) + jnp.dot(halo_adj, remote_rows, preferred_element_type=jnp.float32)

    return lax.map(one_device, blocks).reshape(GROUP_SIZE * NODES_DEV, feat_width)


def aggregate_back(a_int, a_halo, grad_rows, send_idx):
    feat_width = grad_rows.shape[-1]
    local_rows = grad_rows.reshape(GROUP_SIZE, NODES_DEV, feat_width)
    blocks = (a_int.reshape(GROUP_SIZE, NODES_DEV, NODES_DEV), a_halo.reshape(GROUP_SIZE, NODES_DEV, NUM_LINKS * HALO_SLOTS), local_rows)

    def one_device(block):
        inner_adj, halo_adj, own_rows = block
        inner_sum = jnp.dot(inner_adj.T, own_rows, preferred_element_type=jnp.float32)
        outward = jnp.dot(halo_adj.T, own_rows, preferred_element_type=jnp.float32).astype(jnp.bfloat16)
        return inner_sum, outward

    inner_sum, outward = lax.map(one_device, blocks)
    outward = outward.reshape(GROUP_SIZE, NUM_LINKS, HALO_SLOTS, feat_width)
    returned = jnp.stack([jnp.roll(outward[:, link], -OFFSETS[link], axis=0) for link in range(NUM_LINKS)], axis=1)
    returned = returned.reshape(GROUP_SIZE, NUM_LINKS * HALO_SLOTS, feat_width)
    send_plan = send_idx.reshape(GROUP_SIZE, NUM_LINKS * HALO_SLOTS)
    total_sum = jax.vmap(lambda sums_dev, plan_dev, rows_dev: sums_dev.at[plan_dev].add(rows_dev.astype(jnp.float32)))(inner_sum, send_plan, returned)
    return total_sum.reshape(GROUP_SIZE * NODES_DEV, feat_width)


def reference(node_feats, a_int, a_halo, send_idx, w_first, w_second, grad_out):
    z_first = aggregate(a_int, a_halo, node_feats, send_idx).astype(jnp.bfloat16)
    hidden = jnp.maximum(jnp.dot(z_first, w_first, preferred_element_type=jnp.float32), 0.0).astype(jnp.bfloat16)
    z_second = aggregate(a_int, a_halo, hidden, send_idx).astype(jnp.bfloat16)
    dw_second = jnp.dot(z_second.T, grad_out, preferred_element_type=jnp.float32)
    dz_second = jnp.dot(grad_out, w_second.T, preferred_element_type=jnp.float32).astype(jnp.bfloat16)
    d_hidden = aggregate_back(a_int, a_halo, dz_second, send_idx)
    grad_pre = jnp.where(hidden > 0, d_hidden, 0.0).astype(jnp.bfloat16)
    dw_first = jnp.dot(z_first.T, grad_pre, preferred_element_type=jnp.float32)
    dz_first = jnp.dot(grad_pre, w_first.T, preferred_element_type=jnp.float32).astype(jnp.bfloat16)
    grad_feats = aggregate_back(a_int, a_halo, dz_first, send_idx)
    return (dw_first, dw_second, grad_feats)
```

```python
import functools

import jax
import jax.numpy as jnp
from jax import lax
from jax.experimental import pallas as pl
from jax.experimental.pallas import tpu as pltpu
from jax.sharding import PartitionSpec as P

BF = jnp.bfloat16
F32 = jnp.float32
OFFSETS = (1, -1, 2, -2)
SLOTS = 128
CHUNKS = 64
ANY = pl.BlockSpec(memory_space=pl.ANY)


def torus_dims(n):
    return {128: (4, 4, 4, 2), 16: (2, 2, 2, 2)}[n]


def dot(a, b):
    return jnp.dot(a, b, preferred_element_type=F32)


def dot_nt(a, b):
    return lax.dot_general(a, b, (((1,), (1,)), ((), ())), preferred_element_type=F32)


def blocks(total, block, body):
    if total <= block:
        body(pl.ds(0, total))
        return

    @pl.loop(0, total // block)
    def _(i):
        body(pl.ds(pl.multiple_of(i * block, block), block))


def kernel(n, x_hbm, aint_hbm, ahalo_hbm, idx_hbm, w0_hbm, w1_hbm, g_hbm, dw1_hbm, dw2_hbm, gf_hbm,
           x, aint, ahalo, idx, w0, w1, g, s, e1t, o1, r1, g0, h0, zpart, d1t, z0, h1, h1t, g1, hh1, z1part,
           w0t, gt, ft, e0t, o0, r0, gfacc, gfout, dw1out, dw2out,
           ar, res, rs1, rs2, load_sem, out_sem, halo_send, halo_recv, p1s, p1r, p2s, p2r, p3s, p3r, p4s, p4r):
    dims = torus_dims(n)
    nz, ny, nx, nc = dims
    strides = (ny * nx * nc, nx * nc, nc, 1)
    me = lax.axis_index("nodes")
    pos = [lax.rem(lax.div(me, st), d) for st, d in zip(strides, dims)]
    core = pos[3]

    def at(delta):
        return sum(lax.rem(pos[a] + delta[a], dims[a]) * strides[a] for a in range(4))

    near = set()
    for dz in range(nz):
        for dy in range(ny):
            for dx in range(nx):
                moved = (dz > 0) + (dy > 0) + (dx > 0)
                if 0 < moved < 3:
                    near.add((dz, dy, dx, 0))
                if moved <= 1:
                    near.add((dz, dy, dx, 1))
    near = sorted(near)
    partners = [lax.rem(me + o + n, n) for o in OFFSETS]

    barrier = pltpu.get_barrier_semaphore()
    for d in partners + [at(delta) for delta in near]:
        pl.semaphore_signal(barrier, inc=1, device_id={"nodes": d})

    loads = [pltpu.make_async_copy(src, dst, load_sem.at[i]) for i, (src, dst) in enumerate([
        (idx_hbm, idx), (x_hbm, x), (w1_hbm, w1), (g_hbm, g), (ahalo_hbm, ahalo), (aint_hbm, aint), (w0_hbm, w0)])]
    for load in loads:
        load.start()

    def halo_copies(which, src, dst, sign):
        return [pltpu.make_async_remote_copy(
            src_ref=src(k), dst_ref=dst(k), send_sem=halo_send.at[which, k], recv_sem=halo_recv.at[which, k],
            device_id={"nodes": lax.rem(me + sign * o + n, n)}) for k, o in enumerate(OFFSETS)]

    rows = lambda k: pl.ds(k * SLOTS, SLOTS)
    copy_h0 = halo_copies(0, lambda k: g0.at[rows(k)], lambda k: h0.at[rows(k)], 1)
    copy_d1 = halo_copies(1, lambda k: o1.at[k], lambda k: r1.at[k], -1)
    copy_h1 = halo_copies(2, lambda k: g1.at[rows(k)], lambda k: hh1.at[rows(k)], 1)
    copy_d0 = halo_copies(3, lambda k: o0.at[k], lambda k: r0.at[k], -1)

    nodes = x.shape[0]
    loads[0].wait()
    lane = lax.broadcasted_iota(jnp.int32, (SLOTS, SLOTS), 1)
    for k in range(4):
        col = jnp.broadcast_to(idx[k:k + 1, :], (SLOTS, SLOTS)).T
        for b in range(nodes // SLOTS):
            s[rows(k), b * SLOTS:(b + 1) * SLOTS] = jnp.where(col == lane + b * SLOTS, 1.0, 0.0).astype(BF)

    loads[1].wait()
    g0[...] = dot(s[...], x[...]).astype(BF)
    pl.semaphore_wait(barrier, len(partners) + len(near))
    for copy in copy_h0:
        copy.start()

    loads[2].wait()
    loads[3].wait()

    def make_e1(r):
        e1t[r] = dot_nt(w1[r], g[...]).astype(BF)
    blocks(w1.shape[0], 256, make_e1)
    loads[4].wait()

    def make_o1(r):
        out = dot(e1t[r], ahalo[...]).astype(BF)
        for k in range(4):
            o1[k, r] = out[:, k * SLOTS:(k + 1) * SLOTS]
    blocks(w1.shape[0], 256, make_o1)
    for copy in copy_d1:
        copy.start()

    loads[5].wait()
    loads[6].wait()

    def make_zpart(r):
        zpart[r] = dot(aint[r], x[...])
    blocks(nodes, 256, make_zpart)

    feats = x.shape[1]
    z0[:, 128:] = jnp.zeros((nodes, 128), BF)
    pad = jnp.zeros((256 - feats, w0.shape[1]), F32)
    w0t[...] = jnp.concatenate([w0[...].astype(F32), pad], axis=0).T.astype(BF)
    classes = g.shape[1]
    gt[...] = jnp.zeros(gt.shape, BF)
    gt[0:classes, :] = g[...].astype(F32).T.astype(BF)

    for copy in copy_h0:
        copy.wait_recv()

    def make_h1(r):
        z = (zpart[r] + dot(ahalo[r], h0[...])).astype(BF)
        z0[r, 0:feats] = z
        h1[r] = jnp.maximum(dot(z, w0[...]), 0.0).astype(BF)
    blocks(nodes, 256, make_h1)

    def make_g1(r):
        g1[r] = dot(s[r], h1[...]).astype(BF)
    blocks(4 * SLOTS, 256, make_g1)
    for copy in copy_h1:
        copy.start()

    def make_d1(r):
        d1t[r] = dot(e1t[r], aint[...])
    blocks(w1.shape[0], 256, make_d1)

    def make_h1t(r):
        h1t[r] = jnp.maximum(dot_nt(w0t[r], z0[...]), 0.0).astype(BF)
    blocks(w1.shape[0], 256, make_h1t)

    for copy in copy_d1:
        copy.wait_recv()

    def make_ft(r):
        back = jnp.concatenate([r1[k, r] for k in range(4)], axis=1)
        d1 = d1t[r] + dot(back, s[...])
        ft[r] = jnp.where(h1t[r] > 0, d1, 0.0).astype(BF)
    blocks(w1.shape[0], 256, make_ft)

    def line_of(b):
        return (1, 2, 0)[b]

    def group_size(b):
        return dims[line_of(b)] * nc

    def group_dev(b, q):
        a = line_of(b)
        return me - pos[a] * strides[a] - core + lax.div(q, nc) * strides[a] + lax.rem(q, nc)

    def plane_axes(b):
        return [a for a in range(3) if a != line_of(b)]

    def plane_size(b):
        u, v = plane_axes(b)
        return dims[u] * dims[v]

    def plane_dev(b, p):
        u, v = plane_axes(b)
        return (me - pos[u] * strides[u] - pos[v] * strides[v] + lax.div(p, dims[v]) * strides[u] + lax.rem(p, dims[v]) * strides[v])

    class Sum:
        def __init__(self, b):
            self.b = b
            self.gs, self.ps = group_size(b), plane_size(b)
            self.piece = CHUNKS // self.gs
            self.owners = min(self.piece, self.ps)
            self.part = self.piece // self.owners
            self.q = pos[line_of(b)] * nc + core
            u, v = plane_axes(b)
            self.p = pos[u] * dims[v] + pos[v]

        def copy1(self, d):
            b = self.b
            to = lax.rem(self.q + d, self.gs)
            return pltpu.make_async_remote_copy(
                src_ref=ar.at[b, pl.ds(to * self.piece, self.piece)], dst_ref=rs1.at[b, d - 1],
                send_sem=p1s.at[b, d - 1], recv_sem=p1r.at[b, d - 1], device_id={"nodes": group_dev(b, to)})

        def copy2(self, d):
            b = self.b
            to = lax.rem(self.p + d, self.ps)
            first = self.q * self.piece + lax.rem(to, self.owners) * self.part
            return to, pltpu.make_async_remote_copy(
                src_ref=ar.at[b, pl.ds(first, self.part)], dst_ref=rs2.at[b, d - 1],
                send_sem=p2s.at[b, d - 1], recv_sem=p2r.at[b, d - 1], device_id={"nodes": plane_dev(b, to)})

        def copy3(self, d):
            b = self.b
            to = lax.rem(self.p + d, self.ps)
            mine = pl.ds(self.q * self.piece + lax.rem(self.p, self.owners) * self.part, self.part)
            return pltpu.make_async_remote_copy(
                src_ref=res.at[b, mine], dst_ref=res.at[b, mine],
                send_sem=p3s.at[b, d - 1], recv_sem=p3r.at[b, d - 1], device_id={"nodes": plane_dev(b, to)})

        def copy4(self, d):
            b = self.b
            to = lax.rem(self.q + d, self.gs)
            mine = pl.ds(self.q * self.piece, self.piece)
            return pltpu.make_async_remote_copy(
                src_ref=res.at[b, mine], dst_ref=res.at[b, mine],
                send_sem=p4s.at[b, d - 1], recv_sem=p4r.at[b, d - 1], device_id={"nodes": group_dev(b, to)})

        def start1(self):
            for d in range(1, self.gs):
                self.copy1(d).start()

        def step2(self):
            for d in range(1, self.gs):
                self.copy1(d).wait()
            mine = pl.ds(self.q * self.piece, self.piece)
            ar[self.b, mine] = ar[self.b, mine] + jnp.sum(rs1[self.b], axis=0)
            for d in range(1, self.ps):
                to, copy = self.copy2(d)

                @pl.when(to < self.owners)
                def _():
                    copy.start()

        def step3(self):
            for d in range(1, self.ps):
                to, copy = self.copy2(d)

                @pl.when(to < self.owners)
                def _():
                    copy.wait_send()

            @pl.when(self.p < self.owners)
            def _():
                for d in range(1, self.ps):
                    self.copy2(d)[1].wait_recv()
                mine = pl.ds(self.q * self.piece + lax.rem(self.p, self.owners) * self.part, self.part)
                res[self.b, mine] = ar[self.b, mine] + jnp.sum(rs2[self.b], axis=0)
                for d in range(1, self.ps):
                    self.copy3(d).start()

        def step4(self):
            for d in range(1, self.ps):
                source = lax.rem(self.p - d + self.ps, self.ps)

                @pl.when(source < self.owners)
                def _():
                    self.copy3(d).wait_recv()

            @pl.when(self.p < self.owners)
            def _():
                for d in range(1, self.ps):
                    self.copy3(d).wait_send()
            for d in range(1, self.gs):
                self.copy4(d).start()

        def finish(self):
            for d in range(1, self.gs):
                self.copy4(d).wait()

    sums = [Sum(b) for b in range(3)]

    def make_dw1(r):
        part = dot(ft[r], z0[...])
        chunk = pl.ds(lax.div(r.start, 8) if not isinstance(r.start, int) else r.start // 8, r.size // 8)
        ar[0, chunk] = part[:, 0:128].reshape(r.size // 8, 8, 128)
        ar[1, chunk] = part[:, 128:256].reshape(r.size // 8, 8, 128)
    blocks(w1.shape[0], 256, make_dw1)
    sums[0].start1()
    sums[1].start1()

    e0t[...] = dot(w0[...], ft[...]).astype(BF)
    out0 = dot(e0t[...], ahalo[...]).astype(BF)
    for k in range(4):
        o0[k] = out0[:, k * SLOTS:(k + 1) * SLOTS]
    for copy in copy_d0:
        copy.start()

    def make_z1part(r):
        z1part[r] = dot(aint[r], h1[...])
    blocks(nodes, 256, make_z1part)

    for copy in copy_h1:
        copy.wait_recv()

    def make_z1(r):
        h1[r] = (z1part[r] + dot(ahalo[r], hh1[...])).astype(BF)
    blocks(nodes, 256, make_z1)
    dw2t = dot(gt[...], h1[...])
    for b in range(4):
        ar[2, b * 16:(b + 1) * 16] = dw2t[:, b * 128:(b + 1) * 128].reshape(16, 8, 128)
    sums[2].start1()

    sums[0].step2()
    sums[1].step2()
    gfacc[0:feats, :] = dot(e0t[...], aint[...])
    sums[2].step2()
    for copy in copy_d0:
        copy.wait_recv()
    back0 = jnp.concatenate([r0[k] for k in range(4)], axis=1)
    gfacc[0:feats, :] = gfacc[0:feats, :] + dot(back0, s[...])
    sums[0].step3()
    sums[1].step3()
    gfacc[feats:, :] = jnp.zeros((256 - feats, nodes), F32)
    gfout[...] = gfacc[...].T[:, 0:feats]
    out_gf = pltpu.make_async_copy(gfout, gf_hbm, out_sem.at[0])
    out_gf.start()
    sums[2].step3()
    sums[0].step4()
    sums[1].step4()
    sums[2].step4()
    sums[0].finish()
    sums[1].finish()
    dw1out[0:128, :] = res[0].reshape(512, 128).T
    dw1out[128:feats, :] = res[1].reshape(512, 128).T[0:feats - 128, :]
    out_dw1 = pltpu.make_async_copy(dw1out, dw1_hbm, out_sem.at[1])
    out_dw1.start()
    sums[2].finish()
    for b in range(4):
        dw2out[b * 128:(b + 1) * 128, :] = res[2, b * 16:(b + 1) * 16].reshape(128, 128).T[:, 0:classes]
    out_dw2 = pltpu.make_async_copy(dw2out, dw2_hbm, out_sem.at[2])
    out_dw2.start()
    for copy in copy_h0 + copy_d1 + copy_h1 + copy_d0:
        copy.wait_send()
    out_gf.wait()
    out_dw1.wait()
    out_dw2.wait()


def solution(mesh):
    n = mesh.shape["nodes"]
    nz, ny, nx, nc = torus_dims(n)
    group = nx * nc
    plane = nx * ny
    row_spec = P(("graph", "nodes"), None)
    replicated = P(None, None)
    part_spec = P("graph", None)

    def device_step(node_feats, a_int, a_halo, send_idx, w_first, w_second, grad_out):
        nodes, feats = node_feats.shape
        hidden, classes = w_second.shape
        slots = a_halo.shape[1]
        piece = CHUNKS // group
        part = piece // min(piece, plane)
        v = pltpu.VMEM
        dma = pltpu.SemaphoreType.DMA
        return pl.pallas_call(
            functools.partial(kernel, n),
            out_shape=(jax.ShapeDtypeStruct((feats, hidden), F32), jax.ShapeDtypeStruct((hidden, classes), F32),
                       jax.ShapeDtypeStruct((nodes, feats), F32)),
            in_specs=[ANY] * 7,
            out_specs=[ANY] * 3,
            scratch_shapes=[
                v((nodes, feats), BF), v((nodes, nodes), BF), v((nodes, slots), BF), v((4, SLOTS), jnp.int32),
                v((feats, hidden), BF), v((hidden, classes), BF), v((nodes, classes), BF),
                v((slots, nodes), BF),
                v((hidden, nodes), BF),
                v((4, hidden, SLOTS), BF),
                v((4, hidden, SLOTS), BF),
                v((slots, feats), BF),
                v((slots, feats), BF),
                v((nodes, feats), F32),
                v((hidden, nodes), F32),
                v((nodes, 256), BF),
                v((nodes, hidden), BF),
                v((hidden, nodes), BF),
                v((slots, hidden), BF),
                v((slots, hidden), BF),
                v((nodes, hidden), F32),
                v((hidden, 256), BF),
                v((128, nodes), BF),
                v((hidden, nodes), BF),
                v((feats, nodes), BF),
                v((4, feats, SLOTS), BF),
                v((4, feats, SLOTS), BF),
                v((256, nodes), F32),
                v((nodes, feats), F32),
                v((feats, hidden), F32),
                v((hidden, classes), F32),
                v((3, CHUNKS, 8, 128), F32),
                v((3, CHUNKS, 8, 128), F32),
                v((3, group - 1, piece, 8, 128), F32),
                v((3, plane - 1, part, 8, 128), F32),
                dma((7,)), dma((3,)), dma((4, 4)), dma((4, 4)),
                dma((3, group - 1)), dma((3, group - 1)), dma((3, plane - 1)), dma((3, plane - 1)),
                dma((3, plane - 1)), dma((3, plane - 1)), dma((3, group - 1)), dma((3, group - 1)),
            ],
            compiler_params=pltpu.CompilerParams(collective_id=0, has_side_effects=True),
        )(node_feats, a_int, a_halo, send_idx, w_first, w_second, grad_out)

    return jax.shard_map(device_step, mesh=mesh, in_specs=(row_spec, row_spec, row_spec, row_spec, replicated, replicated, row_spec), out_specs=(part_spec, part_spec, row_spec), check_vma=False)
```

```python
import functools

import jax
import jax.numpy as jnp
from jax import lax
from jax.experimental import pallas as pl
from jax.experimental.pallas import tpu as pltpu
from jax.sharding import PartitionSpec as P

BF = jnp.bfloat16
F32 = jnp.float32
OFFSETS = (1, -1, 2, -2)
SLOTS = 128
CHUNKS = 56
USED = (56, 48, 56)
ANY = pl.BlockSpec(memory_space=pl.ANY)


def torus_dims(n):
    return {128: (4, 4, 4, 2), 16: (2, 2, 2, 2)}[n]


def dot(a, b):
    return jnp.dot(a, b, preferred_element_type=F32)


def dot_nt(a, b):
    return lax.dot_general(a, b, (((1,), (1,)), ((), ())), preferred_element_type=F32)


def kernel(n, xt_hbm, aint_hbm, ahalo_hbm, idx_hbm, w0_hbm, w1t_hbm, gt_hbm, dw1_hbm, dw2t_hbm, gft_hbm,
           xt, aint, ahalo, idx, w0, w1t, gt, st, s, e1t, o1, r1, g0, h0, zpart, d1t, z0t, h1t, g1, hh1, z1part, z1t,
           w0t, w1, gtp, ft, e0t, o0, r0, gft, dw1out, dw2out,
           ar, res, rs1, rs2, load_sem, out_sem, halo_send, halo_recv, p1s, p1r, p2s, p2r, p3s, p3r, p4s, p4r):
    dims = torus_dims(n)
    nz, ny, nx, nc = dims
    strides = (ny * nx * nc, nx * nc, nc, 1)
    me = lax.axis_index("nodes")
    pos = [lax.rem(lax.div(me, st_), d) for st_, d in zip(strides, dims)]
    core = pos[3]
    feats, nodes = xt.shape
    classes, hidden = w1t.shape

    def at(delta):
        return sum(lax.rem(pos[a] + delta[a], dims[a]) * strides[a] for a in range(4))

    near = set()
    for dz in range(nz):
        for dy in range(ny):
            for dx in range(nx):
                moved = (dz > 0) + (dy > 0) + (dx > 0)
                if 0 < moved < 3:
                    near.add((dz, dy, dx, 0))
                if moved <= 1:
                    near.add((dz, dy, dx, 1))
    near = sorted(near)
    partners = [lax.rem(me + o + n, n) for o in OFFSETS]

    barrier = pltpu.get_barrier_semaphore()
    for d in partners + [at(delta) for delta in near]:
        pl.semaphore_signal(barrier, inc=1, device_id={"nodes": d})

    loads = [pltpu.make_async_copy(src, dst, load_sem.at[i]) for i, (src, dst) in enumerate([
        (idx_hbm, idx), (xt_hbm, xt), (w1t_hbm, w1t), (gt_hbm, gt), (ahalo_hbm, ahalo), (aint_hbm, aint), (w0_hbm, w0)])]
    for load in loads:
        load.start()

    def halo_copies(which, src, dst, sign):
        return [pltpu.make_async_remote_copy(
            src_ref=src(k), dst_ref=dst(k), send_sem=halo_send.at[which, k], recv_sem=halo_recv.at[which, k],
            device_id={"nodes": lax.rem(me + sign * o + n, n)}) for k, o in enumerate(OFFSETS)]

    copy_h0 = halo_copies(0, lambda k: g0.at[k], lambda k: h0.at[k], 1)
    copy_d1 = halo_copies(1, lambda k: o1.at[k], lambda k: r1.at[k], -1)
    copy_h1 = halo_copies(2, lambda k: g1.at[k], lambda k: hh1.at[k], 1)
    copy_d0 = halo_copies(3, lambda k: o0.at[k], lambda k: r0.at[k], -1)

    def put(ref, value):
        for k in range(4):
            ref[k] = value[:, k * SLOTS:(k + 1) * SLOTS].astype(BF)

    def take(ref):
        return jnp.concatenate([ref[k] for k in range(4)], axis=1)

    loads[0].wait()
    sub = lax.broadcasted_iota(jnp.int32, (nodes, SLOTS), 0)
    for k in range(4):
        row = jnp.broadcast_to(idx[k:k + 1, :], (nodes, SLOTS))
        st[:, k * SLOTS:(k + 1) * SLOTS] = jnp.where(row == sub, 1.0, 0.0).astype(BF)

    loads[1].wait()
    put(g0, dot(xt[...], st[...]))
    pl.semaphore_wait(barrier, len(partners) + len(near))
    for copy in copy_h0:
        copy.start()

    loads[2].wait()
    loads[3].wait()
    w1[...] = jnp.concatenate([w1t[...].astype(F32), jnp.zeros((128 - classes, hidden), F32)], axis=0).T.astype(BF)
    gtp[...] = jnp.concatenate([gt[...].astype(F32), jnp.zeros((128 - classes, nodes), F32)], axis=0).astype(BF)
    e1t[...] = dot(w1[...], gtp[...]).astype(BF)
    loads[4].wait()
    put(o1, dot(e1t[...], ahalo[...]))
    for copy in copy_d1:
        copy.start()

    loads[5].wait()
    loads[6].wait()
    zpart[...] = dot_nt(xt[...], aint[...])
    w0t[...] = w0[...].astype(F32).T.astype(BF)
    lane = lax.broadcasted_iota(jnp.int32, (SLOTS, SLOTS), 1)
    for k in range(4):
        col = jnp.broadcast_to(idx[k:k + 1, :], (SLOTS, SLOTS)).T
        for b in range(nodes // SLOTS):
            s[k * SLOTS:(k + 1) * SLOTS, b * SLOTS:(b + 1) * SLOTS] = jnp.where(col == lane + b * SLOTS, 1.0, 0.0).astype(BF)

    for copy in copy_h0:
        copy.wait_recv()
    z0t[...] = (zpart[...] + dot_nt(take(h0), ahalo[...])).astype(BF)
    h1t[...] = jnp.maximum(dot(w0t[...], z0t[...]), 0.0).astype(BF)
    put(g1, dot(h1t[...], st[...]))
    for copy in copy_h1:
        copy.start()

    d1t[...] = dot(e1t[...], aint[...])

    for copy in copy_d1:
        copy.wait_recv()
    d1 = d1t[...] + dot(take(r1), s[...])
    ft[...] = jnp.where(h1t[...] > 0, d1, 0.0).astype(BF)

    def line_of(b):
        return (1, 2, 0)[b]

    def group_size(b):
        return dims[line_of(b)] * nc

    def group_dev(b, q):
        a = line_of(b)
        return me - pos[a] * strides[a] - core + lax.div(q, nc) * strides[a] + lax.rem(q, nc)

    def plane_axes(b):
        return [a for a in range(3) if a != line_of(b)]

    def plane_size(b):
        u, v = plane_axes(b)
        return dims[u] * dims[v]

    def plane_dev(b, p):
        u, v = plane_axes(b)
        return (me - pos[u] * strides[u] - pos[v] * strides[v] + lax.div(p, dims[v]) * strides[u] + lax.rem(p, dims[v]) * strides[v])

    class Sum:
        def __init__(self, b):
            self.b = b
            self.gs, self.ps = group_size(b), plane_size(b)
            self.piece, self.owners = shares(b, self.gs, self.ps)
            self.part = self.piece // self.owners
            self.q = pos[line_of(b)] * nc + core
            u, v = plane_axes(b)
            self.p = pos[u] * dims[v] + pos[v]

        def copy1(self, d):
            b = self.b
            to = lax.rem(self.q + d, self.gs)
            return pltpu.make_async_remote_copy(
                src_ref=ar.at[b, pl.ds(to * self.piece, self.piece)], dst_ref=rs1.at[b, d - 1, pl.ds(0, self.piece)],
                send_sem=p1s.at[b, d - 1], recv_sem=p1r.at[b, d - 1], device_id={"nodes": group_dev(b, to)})

        def copy2(self, d):
            b = self.b
            to = lax.rem(self.p + d, self.ps)
            first = self.q * self.piece + lax.rem(to, self.owners) * self.part
            return to, pltpu.make_async_remote_copy(
                src_ref=ar.at[b, pl.ds(first, self.part)], dst_ref=rs2.at[b, d - 1, pl.ds(0, self.part)],
                send_sem=p2s.at[b, d - 1], recv_sem=p2r.at[b, d - 1], device_id={"nodes": plane_dev(b, to)})

        def copy3(self, d):
            b = self.b
            to = lax.rem(self.p + d, self.ps)
            mine = pl.ds(self.q * self.piece + lax.rem(self.p, self.owners) * self.part, self.part)
            return pltpu.make_async_remote_copy(
                src_ref=res.at[b, mine], dst_ref=res.at[b, mine],
                send_sem=p3s.at[b, d - 1], recv_sem=p3r.at[b, d - 1], device_id={"nodes": plane_dev(b, to)})

        def copy4(self, d):
            b = self.b
            to = lax.rem(self.q + d, self.gs)
            mine = pl.ds(self.q * self.piece, self.piece)
            return pltpu.make_async_remote_copy(
                src_ref=res.at[b, mine], dst_ref=res.at[b, mine],
                send_sem=p4s.at[b, d - 1], recv_sem=p4r.at[b, d - 1], device_id={"nodes": group_dev(b, to)})

        def start1(self):
            for d in range(1, self.gs):
                self.copy1(d).start()

        def step2(self):
            for d in range(1, self.gs):
                self.copy1(d).wait()
            mine = pl.ds(self.q * self.piece, self.piece)
            ar[self.b, mine] = ar[self.b, mine] + jnp.sum(rs1[self.b, :, 0:self.piece], axis=0)
            for d in range(1, self.ps):
                to, copy = self.copy2(d)

                @pl.when(to < self.owners)
                def _():
                    copy.start()

        def step3(self):
            for d in range(1, self.ps):
                to, copy = self.copy2(d)

                @pl.when(to < self.owners)
                def _():
                    copy.wait_send()

            @pl.when(self.p < self.owners)
            def _():
                for d in range(1, self.ps):
                    self.copy2(d)[1].wait_recv()
                mine = pl.ds(self.q * self.piece + lax.rem(self.p, self.owners) * self.part, self.part)
                res[self.b, mine] = ar[self.b, mine] + jnp.sum(rs2[self.b, :, 0:self.part], axis=0)
                for d in range(1, self.ps):
                    self.copy3(d).start()

        def step4(self):
            for d in range(1, self.ps):
                source = lax.rem(self.p - d + self.ps, self.ps)

                @pl.when(source < self.owners)
                def _():
                    self.copy3(d).wait_recv()

            @pl.when(self.p < self.owners)
            def _():
                for d in range(1, self.ps):
                    self.copy3(d).wait_send()
            for d in range(1, self.gs):
                self.copy4(d).start()

        def finish(self):
            for d in range(1, self.gs):
                self.copy4(d).wait()

    sums = [Sum(b) for b in range(3)]

    def chunks(value, groups):
        return value.reshape(groups, 8, 128)

    dw1 = dot_nt(z0t[...], ft[...])
    for k in range(4):
        lanes = slice(k * 128, (k + 1) * 128)
        ar[0, k * 14:(k + 1) * 14] = chunks(dw1[0:112, lanes], 14)
        ar[1, k * 11:(k + 1) * 11] = chunks(dw1[112:200, lanes], 11)
    ar[1, 44:48] = jnp.zeros((4, 8, 128), F32)
    sums[0].start1()
    sums[1].start1()

    e0t[...] = dot(w0[...], ft[...]).astype(BF)
    put(o0, dot(e0t[...], ahalo[...]))
    for copy in copy_d0:
        copy.start()

    z1part[...] = dot_nt(h1t[...], aint[...])

    for copy in copy_h1:
        copy.wait_recv()
    z1t[...] = (z1part[...] + dot_nt(take(hh1), ahalo[...])).astype(BF)
    dw2t = dot_nt(gtp[...], z1t[...])
    for k in range(4):
        ar[2, k * 14:(k + 1) * 14] = chunks(dw2t[0:112, k * 128:(k + 1) * 128], 14)
    sums[2].start1()

    sums[0].step2()
    sums[1].step2()
    gft[...] = dot(e0t[...], aint[...])
    sums[2].step2()
    for copy in copy_d0:
        copy.wait_recv()
    gft[...] = gft[...] + dot(take(r0), s[...])
    out_gf = pltpu.make_async_copy(gft, gft_hbm, out_sem.at[0])
    out_gf.start()
    sums[0].step3()
    sums[1].step3()
    sums[2].step3()
    sums[0].step4()
    sums[1].step4()
    sums[2].step4()
    sums[0].finish()
    sums[1].finish()
    for k in range(4):
        lanes = slice(k * 128, (k + 1) * 128)
        dw1out[0:112, lanes] = res[0, k * 14:(k + 1) * 14].reshape(112, 128)
        dw1out[112:200, lanes] = res[1, k * 11:(k + 1) * 11].reshape(88, 128)
    out_dw1 = pltpu.make_async_copy(dw1out, dw1_hbm, out_sem.at[1])
    out_dw1.start()
    sums[2].finish()
    for k in range(4):
        dw2out[:, k * 128:(k + 1) * 128] = res[2, k * 14:(k + 1) * 14].reshape(112, 128)[0:classes]
    out_dw2 = pltpu.make_async_copy(dw2out, dw2t_hbm, out_sem.at[2])
    out_dw2.start()
    for copy in copy_h0 + copy_d1 + copy_h1 + copy_d0:
        copy.wait_send()
    out_gf.wait()
    out_dw1.wait()
    out_dw2.wait()


def shares(b, group, plane):
    piece = USED[b] // group
    return piece, max(d for d in range(1, plane + 1) if piece % d == 0)


def solution(mesh):
    n = mesh.shape["nodes"]
    nz, ny, nx, nc = torus_dims(n)
    group = nx * nc
    plane = nx * ny
    row_spec = P(("graph", "nodes"), None)
    replicated = P(None, None)
    part_spec = P("graph", None)

    def device_step(node_feats, a_int, a_halo, send_idx, w_first, w_second, grad_out):
        nodes, feats = node_feats.shape
        hidden, classes = w_second.shape
        slots = a_halo.shape[1]
        piece = CHUNKS // group
        part = max(shares(b, group, plane)[0] // shares(b, group, plane)[1] for b in range(3))
        v = pltpu.VMEM
        dma = pltpu.SemaphoreType.DMA
        dw1, dw2t, gft = pl.pallas_call(
            functools.partial(kernel, n),
            out_shape=(jax.ShapeDtypeStruct((feats, hidden), F32), jax.ShapeDtypeStruct((classes, hidden), F32),
                       jax.ShapeDtypeStruct((feats, nodes), F32)),
            in_specs=[ANY] * 7,
            out_specs=[ANY] * 3,
            scratch_shapes=[
                v((feats, nodes), BF),
                v((nodes, nodes), BF),
                v((nodes, slots), BF),
                v((4, SLOTS), jnp.int32),
                v((feats, hidden), BF),
                v((classes, hidden), BF),
                v((classes, nodes), BF),
                v((nodes, slots), BF),
                v((slots, nodes), BF),
                v((hidden, nodes), BF),
                v((4, hidden, SLOTS), BF),
                v((4, hidden, SLOTS), BF),
                v((4, feats, SLOTS), BF),
                v((4, feats, SLOTS), BF),
                v((feats, nodes), F32),
                v((hidden, nodes), F32),
                v((feats, nodes), BF),
                v((hidden, nodes), BF),
                v((4, hidden, SLOTS), BF),
                v((4, hidden, SLOTS), BF),
                v((hidden, nodes), F32),
                v((hidden, nodes), BF),
                v((hidden, feats), BF),
                v((hidden, 128), BF),
                v((128, nodes), BF),
                v((hidden, nodes), BF),
                v((feats, nodes), BF),
                v((4, feats, SLOTS), BF),
                v((4, feats, SLOTS), BF),
                v((feats, nodes), F32),
                v((feats, hidden), F32),
                v((classes, hidden), F32),
                v((3, CHUNKS, 8, 128), F32),
                v((3, CHUNKS, 8, 128), F32),
                v((3, group - 1, piece, 8, 128), F32),
                v((3, plane - 1, part, 8, 128), F32),
                dma((7,)), dma((3,)), dma((4, 4)), dma((4, 4)),
                dma((3, group - 1)), dma((3, group - 1)), dma((3, plane - 1)), dma((3, plane - 1)),
                dma((3, plane - 1)), dma((3, plane - 1)), dma((3, group - 1)), dma((3, group - 1)),
            ],
            compiler_params=pltpu.CompilerParams(collective_id=0, has_side_effects=True),
        )(node_feats.T, a_int, a_halo, send_idx, w_first, w_second.T, grad_out.T)
        return dw1, dw2t.T, gft.T

    return jax.shard_map(device_step, mesh=mesh, in_specs=(row_spec, row_spec, row_spec, row_spec, replicated, replicated, row_spec), out_specs=(part_spec, part_spec, row_spec), check_vma=False)
```

```python
import functools

import jax
import jax.numpy as jnp
from jax import lax
from jax.experimental import pallas as pl
from jax.experimental.pallas import tpu as pltpu
from jax.sharding import PartitionSpec as P

BF = jnp.bfloat16
F32 = jnp.float32
OFFSETS = (1, -1, 2, -2)
SLOTS = 128
ANY = pl.BlockSpec(memory_space=pl.ANY)
VMEM = pl.BlockSpec(memory_space=pltpu.VMEM)
STAGES = (
    (("rs", "c"), ("rs", "zyx"), ("ag", "zyx"), ("ag", "c")),
    (("rs", "zyc"), ("bc", "x"), ("ag", "zyc")),
)
AXES = "zyxc"


def torus_dims(n):
    return {128: (4, 4, 4, 2), 16: (2, 2, 2, 2)}[n]


def dot(a, b):
    return jnp.dot(a, b, preferred_element_type=F32)


def dot_nt(a, b):
    return lax.dot_general(a, b, (((1,), (1,)), ((), ())), preferred_element_type=F32)


def plan(dims, stages, count):
    out, stack = [], []
    for kind, axes in stages:
        size = 1
        for a in axes:
            size *= dims[AXES.index(a)]
        if kind == "rs":
            piece = next(p for p in range(-(-count // size), count + 1) if count % p == 0)
            owners = count // piece
            out.append((kind, axes, size, owners, piece, (size - 1) * piece))
            stack.append((count, owners))
            count = piece
        elif kind == "bc":
            out.append((kind, axes, size, size, count, size * count))
        else:
            whole, owners = stack.pop()
            out.append((kind, axes, size, owners, count, 0))
            count = whole
    return out


def wait_bytes(ref, sem):
    pltpu.make_async_copy(ref, ref, sem).wait()


def when(condition, body):
    if condition is None:
        body()
    else:
        pl.when(condition)(body)


def both(a, b):
    if a is None or b is None:
        return b if a is None else a
    return jnp.logical_and(a, b)


class Sum:
    def __init__(self, me, pos, dims, strides, stages, count, ar, res, rb, send_sem, recv_sem):
        self.me, self.pos, self.dims, self.strides = me, pos, dims, strides
        self.ar, self.res, self.rb, self.send_sem, self.recv_sem = ar, res, rb, send_sem, recv_sem
        self.plan = plan(dims, stages, count)
        self.drains = []
        self.steps = self.run(count)

    def group(self, axes):
        ids = [AXES.index(a) for a in axes]
        p, base = 0, self.me
        for a in ids:
            p = p * self.dims[a] + self.pos[a]
            base = base - self.pos[a] * self.strides[a]

        def device(q):
            out = base
            for a in reversed(ids):
                out = out + lax.rem(q, self.dims[a]) * self.strides[a]
                q = lax.div(q, self.dims[a])
            return out
        return p, device

    def each(self, size, body):
        if size <= 8:
            for d in range(1, size):
                body(d)
        else:
            pl.loop(1, size)(body)

    def step(self):
        next(self.steps, None)

    def run(self, count):
        ar, res, rb = self.ar, self.res, self.rb
        first, active, offset, stack = 0, None, 0, []
        for i, (kind, axes, size, owners, piece, slots) in enumerate(self.plan):
            p, device = self.group(axes)
            send, recv = self.send_sem.at[i], self.recv_sem.at[i]
            to_of = lambda d: lax.rem(p + d, size)
            if kind == "rs":
                full = owners == size

                def start(d):
                    to = to_of(d)
                    copy = pltpu.make_async_remote_copy(
                        src_ref=ar.at[pl.ds(first + to * piece, piece)], dst_ref=rb.at[pl.ds(offset + (d - 1) * piece, piece)],
                        send_sem=send, recv_sem=recv, device_id={"nodes": device(to)})
                    when(None if full else to < owners, copy.start)
                when(active, lambda: self.each(size, start))
                yield
                mine = both(active, None if full else p < owners)
                new = first + p * piece
                got = pl.ds(offset, slots)

                def collect():
                    wait_bytes(rb.at[got], recv)
                    total = ar[pl.ds(new, piece)] + jnp.sum(rb[got].reshape(size - 1, piece, 8, 128), axis=0)
                    ar[pl.ds(new, piece)] = total
                    res[pl.ds(new, piece)] = total
                when(mine, collect)
                if full:
                    self.drains.append((active, send, (size - 1) * piece))
                else:
                    self.drains.append((mine, send, (owners - 1) * piece))
                    self.drains.append((both(active, p >= owners), send, owners * piece))
                stack.append((first, active, p, full))
                first, active = new, mine
                offset += slots
            elif kind == "bc":
                mine = pl.ds(first, piece)

                def start(d):
                    to = to_of(d)
                    pltpu.make_async_remote_copy(
                        src_ref=ar.at[mine], dst_ref=rb.at[pl.ds(offset + p * piece, piece)],
                        send_sem=send, recv_sem=recv, device_id={"nodes": device(to)}).start()

                def spread():
                    self.each(size, start)
                    rb[pl.ds(offset + p * piece, piece)] = ar[mine]
                when(active, spread)
                yield

                def collect():
                    wait_bytes(rb.at[pl.ds(offset, slots - piece)], recv)
                    res[mine] = jnp.sum(rb[pl.ds(offset, slots)].reshape(size, piece, 8, 128), axis=0)
                when(active, collect)
                self.drains.append((active, send, (size - 1) * piece))
                offset += slots
            else:
                mine = pl.ds(first, piece)

                def start(d):
                    pltpu.make_async_remote_copy(
                        src_ref=res.at[mine], dst_ref=res.at[mine],
                        send_sem=send, recv_sem=recv, device_id={"nodes": device(to_of(d))}).start()
                when(active, lambda: self.each(size, start))
                yield
                self.drains.append((active, send, (size - 1) * piece))
                first, active, p, full = stack.pop()
                if full:
                    when(active, lambda: wait_bytes(res.at[pl.ds(0, (size - 1) * piece)], recv))
                else:
                    when(both(active, p < owners), lambda: wait_bytes(res.at[pl.ds(0, (owners - 1) * piece)], recv))
                    when(both(active, p >= owners), lambda: wait_bytes(res.at[pl.ds(0, owners * piece)], recv))

    def drain(self):
        for condition, sem, slots in self.drains:
            when(condition, lambda: wait_bytes(self.rb.at[pl.ds(0, slots)], sem))


def kernel(n, xt_hbm, aint_hbm, ahalo_hbm, idx_hbm, w0_hbm, w1t_hbm, gt_hbm, dw1_ref, dw2t_ref, gft,
           xt, aint, ahalo, idx, w0, w1t, gt, st, s, e1t, o1, r1, g0, h0, zpart, d1t, z0t, h1t, g1, zh, z1part, z1t,
           w0t, w1, gtp, ft, e0t, o0, r0, ar1, res1, rb1, ar2, res2, rb2,
           load_sem, halo_send, halo_recv, send1, recv1, send2, recv2):
    dims = torus_dims(n)
    strides = tuple(dims[i + 1] * dims[i + 2] * dims[i + 3] if i == 0 else (dims[2] * dims[3], dims[3], 1)[i - 1] for i in range(4))
    me = lax.axis_index("nodes")
    pos = [lax.rem(lax.div(me, stride), d) for stride, d in zip(strides, dims)]
    feats, nodes = xt.shape
    classes, hidden = w1t.shape

    barrier = pltpu.get_barrier_semaphore()

    @pl.loop(1, n)
    def _(i):
        pl.semaphore_signal(barrier, inc=1, device_id={"nodes": lax.rem(me + i, n)})

    loads = [pltpu.make_async_copy(src, dst, load_sem.at[i]) for i, (src, dst) in enumerate([
        (idx_hbm, idx), (xt_hbm, xt), (w1t_hbm, w1t), (gt_hbm, gt), (ahalo_hbm, ahalo), (aint_hbm, aint), (w0_hbm, w0)])]
    for load in loads:
        load.start()

    class Halo:
        def __init__(self, which, src, dst, sign):
            self.src, self.dst = src, dst
            self.send, self.recv = halo_send.at[which], halo_recv.at[which]
            self.sign = sign

        def start(self):
            for k, o in enumerate(OFFSETS):
                pltpu.make_async_remote_copy(
                    src_ref=self.src.at[k], dst_ref=self.dst.at[k], send_sem=self.send, recv_sem=self.recv,
                    device_id={"nodes": lax.rem(me + self.sign * o + n, n)}).start()

        def wait_recv(self):
            wait_bytes(self.dst, self.recv)

        def wait_send(self):
            wait_bytes(self.src, self.send)

    halo_x = Halo(0, g0, h0, 1)
    halo_d1 = Halo(1, o1, r1, -1)
    halo_z = Halo(2, g1, zh, 1)
    halo_d0 = Halo(3, o0, r0, -1)
    sum1 = Sum(me, pos, dims, strides, STAGES[0], ar1.shape[0], ar1, res1, rb1, send1, recv1)
    sum2 = Sum(me, pos, dims, strides, STAGES[1], ar2.shape[0], ar2, res2, rb2, send2, recv2)

    def put(ref, value):
        for k in range(4):
            ref[k] = value[:, k * SLOTS:(k + 1) * SLOTS].astype(BF)

    def take(ref):
        return jnp.concatenate([ref[k] for k in range(4)], axis=1)

    loads[0].wait()
    sub = lax.broadcasted_iota(jnp.int32, (nodes, SLOTS), 0)
    for k in range(4):
        row = jnp.broadcast_to(idx[k:k + 1, :], (nodes, SLOTS))
        st[:, k * SLOTS:(k + 1) * SLOTS] = jnp.where(row == sub, 1.0, 0.0).astype(BF)

    loads[1].wait()
    put(g0, dot(xt[...], st[...]))
    loads[2].wait()
    loads[3].wait()
    w1[...] = jnp.concatenate([w1t[...].astype(F32), jnp.zeros((128 - classes, hidden), F32)], axis=0).T.astype(BF)
    gtp[...] = jnp.concatenate([gt[...].astype(F32), jnp.zeros((128 - classes, nodes), F32)], axis=0).astype(BF)
    e1t[...] = dot(w1[...], gtp[...]).astype(BF)
    loads[4].wait()
    put(o1, dot(e1t[...], ahalo[...]))

    pl.semaphore_wait(barrier, n - 1)
    halo_x.start()

    loads[5].wait()
    loads[6].wait()
    zpart[...] = dot_nt(xt[...], aint[...])
    halo_d1.start()
    w0t[...] = w0[...].astype(F32).T.astype(BF)
    lane = lax.broadcasted_iota(jnp.int32, (SLOTS, SLOTS), 1)
    for k in range(4):
        col = jnp.broadcast_to(idx[k:k + 1, :], (SLOTS, SLOTS)).T
        for b in range(nodes // SLOTS):
            s[k * SLOTS:(k + 1) * SLOTS, b * SLOTS:(b + 1) * SLOTS] = jnp.where(col == lane + b * SLOTS, 1.0, 0.0).astype(BF)
    d1t[...] = dot(e1t[...], aint[...])

    def hidden_of(zt):
        return jnp.maximum(dot(w0t[...], zt), 0.0).astype(BF)

    halo_x.wait_recv()
    z0t[...] = (zpart[...] + dot_nt(take(h0), ahalo[...])).astype(BF)
    put(g1, dot(z0t[...], st[...]))
    halo_z.start()
    h1t[...] = hidden_of(z0t[...])
    z1part[...] = dot_nt(h1t[...], aint[...])

    halo_d1.wait_recv()
    d1 = d1t[...] + dot(take(r1), s[...])
    ft[...] = jnp.where(h1t[...] > 0, d1, 0.0).astype(BF)

    def to_chunks(ref, value):
        groups = value.shape[0] // 8
        for k in range(hidden // 128):
            ref[k * groups:(k + 1) * groups] = value[:, k * 128:(k + 1) * 128].reshape(groups, 8, 128)

    def from_chunks(out_ref, ref, rows):
        groups = ref.shape[0] // (hidden // 128)
        for k in range(hidden // 128):
            out_ref[:, k * 128:(k + 1) * 128] = ref[k * groups:(k + 1) * groups].reshape(groups * 8, 128)[0:rows]

    to_chunks(ar1, dot_nt(z0t[...], ft[...]))
    sum1.step()
    e0t[...] = dot(w0[...], ft[...]).astype(BF)
    put(o0, dot(e0t[...], ahalo[...]))
    halo_d0.start()

    halo_z.wait_recv()
    z1t[...] = (z1part[...] + dot_nt(hidden_of(take(zh)), ahalo[...])).astype(BF)
    padded = -(-classes // 8) * 8
    to_chunks(ar2, dot_nt(gtp[...], z1t[...])[0:padded])
    sum2.step()

    sum1.step()
    gft[...] = dot(e0t[...], aint[...])
    sum2.step()
    sum1.step()
    sum2.step()
    halo_d0.wait_recv()
    gft[...] = gft[...] + dot(take(r0), s[...])
    for _ in range(3):
        sum1.step()
    from_chunks(dw1_ref, res1, feats)
    for _ in range(3):
        sum2.step()
    from_chunks(dw2t_ref, res2, classes)
    for halo in (halo_x, halo_d1, halo_z, halo_d0):
        halo.wait_send()
    sum1.drain()
    sum2.drain()


def write_out(a, b, c, x, y, z, sem):
    copies = [pltpu.make_async_copy(src, dst, sem.at[i]) for i, (src, dst) in enumerate([(a, x), (b, y), (c, z)])]
    for copy in copies:
        copy.start()
    for copy in copies:
        copy.wait()


def solution(mesh):
    n = mesh.shape["nodes"]
    dims = torus_dims(n)
    row_spec = P(("graph", "nodes"), None)
    replicated = P(None, None)
    part_spec = P("graph", None)

    def device_step(node_feats, a_int, a_halo, send_idx, w_first, w_second, grad_out):
        nodes, feats = node_feats.shape
        hidden, classes = w_second.shape
        slots = a_halo.shape[1]
        v = pltpu.VMEM
        dma = pltpu.SemaphoreType.DMA
        counts = (feats // 8 * (hidden // 128), -(-classes // 8) * (hidden // 128))
        sums = []
        for stages, count in zip(STAGES, counts):
            sums += [v((count, 8, 128), F32), v((count, 8, 128), F32), v((sum(p[5] for p in plan(dims, stages, count)), 8, 128), F32)]
        outs = pl.pallas_call(
            functools.partial(kernel, n),
            out_shape=(v((feats, hidden), F32), v((classes, hidden), F32), v((feats, nodes), F32)),
            in_specs=[ANY] * 7,
            out_specs=[VMEM] * 3,
            scratch_shapes=[
                v((feats, nodes), BF),
                v((nodes, nodes), BF),
                v((nodes, slots), BF),
                v((4, SLOTS), jnp.int32),
                v((feats, hidden), BF),
                v((classes, hidden), BF),
                v((classes, nodes), BF),
                v((nodes, slots), BF),
                v((slots, nodes), BF),
                v((hidden, nodes), BF),
                v((4, hidden, SLOTS), BF),
                v((4, hidden, SLOTS), BF),
                v((4, feats, SLOTS), BF),
                v((4, feats, SLOTS), BF),
                v((feats, nodes), F32),
                v((hidden, nodes), F32),
                v((feats, nodes), BF),
                v((hidden, nodes), BF),
                v((4, feats, SLOTS), BF),
                v((4, feats, SLOTS), BF),
                v((hidden, nodes), F32),
                v((hidden, nodes), BF),
                v((hidden, feats), BF),
                v((hidden, 128), BF),
                v((128, nodes), BF),
                v((hidden, nodes), BF),
                v((feats, nodes), BF),
                v((4, feats, SLOTS), BF),
                v((4, feats, SLOTS), BF),
                *sums,
                dma((7,)), dma((4,)), dma((4,)),
                dma((len(STAGES[0]),)), dma((len(STAGES[0]),)), dma((len(STAGES[1]),)), dma((len(STAGES[1]),)),
            ],
            compiler_params=pltpu.CompilerParams(collective_id=0, has_side_effects=True, vmem_limit_bytes=40 << 20),
        )(*[pltpu.with_memory_space_constraint(a, pltpu.HBM) for a in
            (node_feats.T, a_int, a_halo, send_idx, w_first, w_second.T, grad_out.T)])
        dw1, dw2t, gft = pl.pallas_call(
            write_out,
            out_shape=tuple(jax.ShapeDtypeStruct(o.shape, F32) for o in outs),
            in_specs=[VMEM] * 3,
            out_specs=[ANY] * 3,
            scratch_shapes=[dma((3,))],
            compiler_params=pltpu.CompilerParams(vmem_limit_bytes=1 << 20),
        )(*outs)
        return dw1, dw2t.T, gft.T

    return jax.shard_map(device_step, mesh=mesh, in_specs=(row_spec, row_spec, row_spec, row_spec, replicated, replicated, row_spec), out_specs=(part_spec, part_spec, row_spec), check_vma=False)
```

```python
import functools

import jax
import jax.numpy as jnp
from jax import lax
from jax.experimental import pallas as pl
from jax.experimental.pallas import tpu as pltpu
from jax.sharding import PartitionSpec as P

BF = jnp.bfloat16
F32 = jnp.float32
OFFSETS = (1, -1, 2, -2)
SLOTS = 128
ANY = pl.BlockSpec(memory_space=pl.ANY)
VMEM = pl.BlockSpec(memory_space=pltpu.VMEM)
FULL = (("rs", "c"), ("rs", "zyx"), ("ag", "zyx"), ("ag", "c"))
PLANE = (("rs", "zy"), ("bc", "xc"), ("ag", "zy"))
SUMS = (
    (1, 0, 4, FULL),
    (2, 0, 4, PLANE),
)
ORDER = "WaEZbagbabdaba"
AXES = "zyxc"


def torus_dims(n):
    return {128: (4, 4, 4, 2), 16: (2, 2, 2, 2)}[n]


def dot(a, b):
    return jnp.dot(a, b, preferred_element_type=F32)


def dot_nt(a, b):
    return lax.dot_general(a, b, (((1,), (1,)), ((), ())), preferred_element_type=F32)


def plan(dims, stages, count):
    out, stack = [], []
    for kind, axes in stages:
        size = 1
        for a in axes:
            size *= dims[AXES.index(a)]
        if kind == "rs":
            piece = next(p for p in range(-(-count // size), count + 1) if count % p == 0)
            owners = count // piece
            out.append((kind, axes, size, owners, piece, (size - 1) * piece))
            stack.append((count, owners))
            count = piece
        elif kind == "bc":
            out.append((kind, axes, size, size, count, size * count))
        else:
            whole, owners = stack.pop()
            out.append((kind, axes, size, owners, count, 0))
            count = whole
    return out


def wait_bytes(ref, sem):
    pltpu.make_async_copy(ref, ref, sem).wait()


def when(condition, body):
    if condition is None:
        body()
    else:
        pl.when(condition)(body)


def both(a, b):
    if a is None or b is None:
        return b if a is None else a
    return jnp.logical_and(a, b)


class Sum:
    def __init__(self, me, pos, dims, strides, stages, count, ar, res, rb, send_sem, recv_sem):
        self.me, self.pos, self.dims, self.strides = me, pos, dims, strides
        self.ar, self.res, self.rb, self.send_sem, self.recv_sem = ar, res, rb, send_sem, recv_sem
        self.plan = plan(dims, stages, count)
        self.drains = []
        self.steps = self.run(count)

    def group(self, axes):
        ids = [AXES.index(a) for a in axes]
        p, base = 0, self.me
        for a in ids:
            p = p * self.dims[a] + self.pos[a]
            base = base - self.pos[a] * self.strides[a]

        def device(q):
            out = base
            for a in reversed(ids):
                out = out + lax.rem(q, self.dims[a]) * self.strides[a]
                q = lax.div(q, self.dims[a])
            return out
        return p, device

    def each(self, size, body, first=1):
        if size <= 8:
            for d in range(first, size):
                body(d)
        else:
            pl.loop(first, size)(body)

    def step(self):
        return next(self.steps, False)

    def run(self, count):
        ar, res, rb = self.ar, self.res, self.rb
        first, active, offset, stack = 0, None, 0, []
        for i, (kind, axes, size, owners, piece, slots) in enumerate(self.plan):
            p, device = self.group(axes)
            send, recv = self.send_sem.at[i], self.recv_sem.at[i]
            to_of = lambda d: lax.rem(p + d, size)
            if kind == "rs":
                full = owners == size

                def start(d):
                    to = to_of(d)
                    copy = pltpu.make_async_remote_copy(
                        src_ref=ar.at[pl.ds(first + to * piece, piece)], dst_ref=rb.at[pl.ds(offset + (d - 1) * piece, piece)],
                        send_sem=send, recv_sem=recv, device_id={"nodes": device(to)})
                    when(None if full else to < owners, copy.start)
                when(active, lambda: self.each(size, start))
                yield True
                mine = both(active, None if full else p < owners)
                new = first + p * piece
                got = pl.ds(offset, slots)

                def collect():
                    wait_bytes(rb.at[got], recv)
                    total = ar[pl.ds(new, piece)] + jnp.sum(rb[got].reshape(size - 1, piece, 8, 128), axis=0)
                    ar[pl.ds(new, piece)] = total
                    res[pl.ds(new, piece)] = total
                when(mine, collect)
                if full:
                    self.drains.append((active, send, (size - 1) * piece))
                else:
                    self.drains.append((mine, send, (owners - 1) * piece))
                    self.drains.append((both(active, p >= owners), send, owners * piece))
                stack.append((first, active, p, full))
                first, active = new, mine
                offset += slots
            elif kind == "bc":
                mine = pl.ds(first, piece)

                def start(d):
                    to = to_of(d)
                    pltpu.make_async_remote_copy(
                        src_ref=ar.at[mine], dst_ref=rb.at[pl.ds(offset + p * piece, piece)],
                        send_sem=send, recv_sem=recv, device_id={"nodes": device(to)}).start()

                def spread():
                    self.each(size, start)
                    rb[pl.ds(offset + p * piece, piece)] = ar[mine]
                when(active, spread)
                yield True

                def collect():
                    wait_bytes(rb.at[pl.ds(offset, slots - piece)], recv)
                    res[mine] = jnp.sum(rb[pl.ds(offset, slots)].reshape(size, piece, 8, 128), axis=0)
                when(active, collect)
                self.drains.append((active, send, (size - 1) * piece))
                offset += slots
            else:
                mine = pl.ds(first, piece)

                def start(to):
                    pl.when(to != p)(pltpu.make_async_remote_copy(
                        src_ref=res.at[mine], dst_ref=res.at[mine],
                        send_sem=send, recv_sem=recv, device_id={"nodes": device(to)}).start)
                when(active, lambda: self.each(size, start, 0))
                yield True
                self.drains.append((active, send, (size - 1) * piece))
                first, active, p, full = stack.pop()
                if full:
                    when(active, lambda: wait_bytes(res.at[pl.ds(0, (size - 1) * piece)], recv))
                else:
                    when(both(active, p < owners), lambda: wait_bytes(res.at[pl.ds(0, (owners - 1) * piece)], recv))
                    when(both(active, p >= owners), lambda: wait_bytes(res.at[pl.ds(0, owners * piece)], recv))

    def drain(self):
        for condition, sem, slots in self.drains:
            when(condition, lambda: wait_bytes(self.rb.at[pl.ds(0, slots)], sem))


def kernel(n, xt_hbm, aint_hbm, ahalo_hbm, idx_hbm, w0_hbm, w1t_hbm, gt_hbm, dw1_ref, dw2t_ref, gft,
           xt, aint, ahalo, idx, w0, w1t, gt, st, s, e1t, o1, r1, g0, h0, zpart, d1t, z0t, h1t, g1, zh, z1part, z1t,
           w0t, w1, gtp, ft, e0t, o0, r0, load_sem, halo_send, halo_recv, *sum_refs):
    dims = torus_dims(n)
    strides = tuple(dims[i + 1] * dims[i + 2] * dims[i + 3] if i == 0 else (dims[2] * dims[3], dims[3], 1)[i - 1] for i in range(4))
    me = lax.axis_index("nodes")
    pos = [lax.rem(lax.div(me, stride), d) for stride, d in zip(strides, dims)]
    feats, nodes = xt.shape
    classes, hidden = w1t.shape

    barrier = pltpu.get_barrier_semaphore()

    @pl.loop(1, n)
    def _(i):
        pl.semaphore_signal(barrier, inc=1, device_id={"nodes": lax.rem(me + i, n)})

    loads = [pltpu.make_async_copy(src, dst, load_sem.at[i]) for i, (src, dst) in enumerate([
        (idx_hbm, idx), (xt_hbm, xt), (w1t_hbm, w1t), (gt_hbm, gt), (ahalo_hbm, ahalo), (aint_hbm, aint), (w0_hbm, w0)])]
    for load in loads:
        load.start()

    class Halo:
        def __init__(self, which, src, dst, sign):
            self.src, self.dst = src, dst
            self.send, self.recv = halo_send.at[which], halo_recv.at[which]
            self.sign = sign

        def start(self):
            for k, o in enumerate(OFFSETS):
                pltpu.make_async_remote_copy(
                    src_ref=self.src.at[k], dst_ref=self.dst.at[k], send_sem=self.send, recv_sem=self.recv,
                    device_id={"nodes": lax.rem(me + self.sign * o + n, n)}).start()

        def wait_recv(self):
            wait_bytes(self.dst, self.recv)

        def wait_send(self):
            wait_bytes(self.src, self.send)

    halo_x = Halo(0, g0, h0, 1)
    halo_d1 = Halo(1, o1, r1, -1)
    halo_z = Halo(2, g1, zh, 1)
    halo_d0 = Halo(3, o0, r0, -1)
    sums = []
    for i, (_, _, _, stages) in enumerate(SUMS):
        refs = sum_refs[5 * i:5 * i + 5]
        sums.append(Sum(me, pos, dims, strides, stages, refs[0].shape[0], *refs))

    def put(ref, value):
        for k in range(4):
            ref[k] = value[:, k * SLOTS:(k + 1) * SLOTS].astype(BF)

    def take(ref):
        return jnp.concatenate([ref[k] for k in range(4)], axis=1)

    loads[0].wait()
    sub = lax.broadcasted_iota(jnp.int32, (nodes, SLOTS), 0)
    for k in range(4):
        row = jnp.broadcast_to(idx[k:k + 1, :], (nodes, SLOTS))
        st[:, k * SLOTS:(k + 1) * SLOTS] = jnp.where(row == sub, 1.0, 0.0).astype(BF)

    loads[1].wait()
    put(g0, dot(xt[...], st[...]))
    loads[2].wait()
    loads[3].wait()
    w1[...] = jnp.concatenate([w1t[...].astype(F32), jnp.zeros((128 - classes, hidden), F32)], axis=0).T.astype(BF)
    gtp[...] = jnp.concatenate([gt[...].astype(F32), jnp.zeros((128 - classes, nodes), F32)], axis=0).astype(BF)
    e1t[...] = dot(w1[...], gtp[...]).astype(BF)
    loads[4].wait()
    put(o1, dot(e1t[...], ahalo[...]))

    pl.semaphore_wait(barrier, n - 1)
    halo_x.start()

    loads[5].wait()
    loads[6].wait()
    zpart[...] = dot_nt(xt[...], aint[...])
    halo_d1.start()
    w0t[...] = w0[...].astype(F32).T.astype(BF)
    lane = lax.broadcasted_iota(jnp.int32, (SLOTS, SLOTS), 1)
    for k in range(4):
        col = jnp.broadcast_to(idx[k:k + 1, :], (SLOTS, SLOTS)).T
        for b in range(nodes // SLOTS):
            s[k * SLOTS:(k + 1) * SLOTS, b * SLOTS:(b + 1) * SLOTS] = jnp.where(col == lane + b * SLOTS, 1.0, 0.0).astype(BF)
    d1t[...] = dot(e1t[...], aint[...])

    def hidden_of(zt):
        return jnp.maximum(dot(w0t[...], zt), 0.0).astype(BF)

    halo_x.wait_recv()
    z0t[...] = (zpart[...] + dot_nt(take(h0), ahalo[...])).astype(BF)
    put(g1, dot(z0t[...], st[...]))
    halo_z.start()
    h1t[...] = hidden_of(z0t[...])
    z1part[...] = dot_nt(h1t[...], aint[...])

    halo_d1.wait_recv()
    d1 = d1t[...] + dot(take(r1), s[...])
    ft[...] = jnp.where(h1t[...] > 0, d1, 0.0).astype(BF)

    def to_chunks(which, value):
        groups = value.shape[0] // 8
        for (weight, lo, hi, _), total in zip(SUMS, sums):
            if weight == which:
                for k in range(lo, hi):
                    total.ar[(k - lo) * groups:(k - lo + 1) * groups] = value[:, k * 128:(k + 1) * 128].reshape(groups, 8, 128)

    def step(i):
        weight, lo, hi, _ = SUMS[i]
        if sums[i].step():
            return
        left.remove(i)
        out_ref, rows = (dw1_ref, feats) if weight == 1 else (dw2t_ref, classes)
        groups = sums[i].res.shape[0] // (hi - lo)
        for k in range(lo, hi):
            out_ref[:, k * 128:(k + 1) * 128] = sums[i].res[(k - lo) * groups:(k - lo + 1) * groups].reshape(groups * 8, 128)[0:rows]

    left = list(range(len(SUMS)))
    for event in ORDER:
        if event == "W":
            to_chunks(1, dot_nt(z0t[...], ft[...]))
        elif event == "E":
            e0t[...] = dot(w0[...], ft[...]).astype(BF)
            put(o0, dot(e0t[...], ahalo[...]))
            halo_d0.start()
        elif event == "Z":
            halo_z.wait_recv()
            z1t[...] = (z1part[...] + dot_nt(hidden_of(take(zh)), ahalo[...])).astype(BF)
            padded = -(-classes // 8) * 8
            to_chunks(2, dot_nt(gtp[...], z1t[...])[0:padded])
        elif event == "g":
            gft[...] = dot(e0t[...], aint[...])
        elif event == "d":
            halo_d0.wait_recv()
            gft[...] = gft[...] + dot(take(r0), s[...])
        else:
            step("abcABC".index(event))
    assert not left
    for halo in (halo_x, halo_d1, halo_z, halo_d0):
        halo.wait_send()
    for total in sums:
        total.drain()


def write_out(a, b, c, x, y, z, sem):
    copies = [pltpu.make_async_copy(src, dst, sem.at[i]) for i, (src, dst) in enumerate([(a, x), (b, y), (c, z)])]
    for copy in copies:
        copy.start()
    for copy in copies:
        copy.wait()


def solution(mesh):
    n = mesh.shape["nodes"]
    dims = torus_dims(n)
    row_spec = P(("graph", "nodes"), None)
    replicated = P(None, None)
    part_spec = P("graph", None)

    def device_step(node_feats, a_int, a_halo, send_idx, w_first, w_second, grad_out):
        nodes, feats = node_feats.shape
        hidden, classes = w_second.shape
        slots = a_halo.shape[1]
        v = pltpu.VMEM
        dma = pltpu.SemaphoreType.DMA
        groups = {1: feats // 8, 2: -(-classes // 8)}
        sum_refs = []
        for weight, lo, hi, stages in SUMS:
            count = groups[weight] * (hi - lo)
            received = sum(p[5] for p in plan(dims, stages, count))
            sum_refs += [v((count, 8, 128), F32), v((count, 8, 128), F32), v((received, 8, 128), F32), dma((len(stages),)), dma((len(stages),))]
        outs = pl.pallas_call(
            functools.partial(kernel, n),
            out_shape=(v((feats, hidden), F32), v((classes, hidden), F32), v((feats, nodes), F32)),
            in_specs=[ANY] * 7,
            out_specs=[VMEM] * 3,
            scratch_shapes=[
                v((feats, nodes), BF),
                v((nodes, nodes), BF),
                v((nodes, slots), BF),
                v((4, SLOTS), jnp.int32),
                v((feats, hidden), BF),
                v((classes, hidden), BF),
                v((classes, nodes), BF),
                v((nodes, slots), BF),
                v((slots, nodes), BF),
                v((hidden, nodes), BF),
                v((4, hidden, SLOTS), BF),
                v((4, hidden, SLOTS), BF),
                v((4, feats, SLOTS), BF),
                v((4, feats, SLOTS), BF),
                v((feats, nodes), F32),
                v((hidden, nodes), F32),
                v((feats, nodes), BF),
                v((hidden, nodes), BF),
                v((4, feats, SLOTS), BF),
                v((4, feats, SLOTS), BF),
                v((hidden, nodes), F32),
                v((hidden, nodes), BF),
                v((hidden, feats), BF),
                v((hidden, 128), BF),
                v((128, nodes), BF),
                v((hidden, nodes), BF),
                v((feats, nodes), BF),
                v((4, feats, SLOTS), BF),
                v((4, feats, SLOTS), BF),
                dma((7,)), dma((4,)), dma((4,)),
                *sum_refs,
            ],
            compiler_params=pltpu.CompilerParams(collective_id=0, has_side_effects=True, vmem_limit_bytes=40 << 20),
        )(*[pltpu.with_memory_space_constraint(a, pltpu.HBM) for a in
            (node_feats.T, a_int, a_halo, send_idx, w_first, w_second.T, grad_out.T)])
        dw1, dw2t, gft = pl.pallas_call(
            write_out,
            out_shape=tuple(jax.ShapeDtypeStruct(o.shape, F32) for o in outs),
            in_specs=[VMEM] * 3,
            out_specs=[ANY] * 3,
            scratch_shapes=[dma((3,))],
            compiler_params=pltpu.CompilerParams(vmem_limit_bytes=1 << 20),
        )(*outs)
        return dw1, dw2t.T, gft.T

    return jax.shard_map(device_step, mesh=mesh, in_specs=(row_spec, row_spec, row_spec, row_spec, replicated, replicated, row_spec), out_specs=(part_spec, part_spec, row_spec), check_vma=False)
```

```python
import functools

import jax
import jax.numpy as jnp
from jax import lax
from jax.experimental import pallas as pl
from jax.experimental.pallas import tpu as pltpu
from jax.sharding import PartitionSpec as P

BF = jnp.bfloat16
F32 = jnp.float32
OFFSETS = (1, -1, 2, -2)
BLOCKS = (0, 2, 1, 3)
ISSUE = (0, 2, 1, 3)
SLOTS = 128
ANY = pl.BlockSpec(memory_space=pl.ANY)
VMEM = pl.BlockSpec(memory_space=pltpu.VMEM)
FULL = (("rs", "c"), ("rs", "zyx"), ("ag", "zyx"), ("ag", "c"))
PLANE = (("rs", "zy"), ("bc", "xc"), ("ag", "zy"))
SUMS = (
    (1, 0, 4, FULL),
    (2, 0, 4, PLANE),
)
ORDER = "WaEZbagbabdaab"
AXES = "zyxc"


def torus_dims(n):
    return {128: (4, 4, 4, 2), 16: (2, 2, 2, 2)}[n]


def dot(a, b):
    return jnp.dot(a, b, preferred_element_type=F32)


def dot_nt(a, b):
    return lax.dot_general(a, b, (((1,), (1,)), ((), ())), preferred_element_type=F32)


def plan(dims, stages, count):
    out, stack = [], []
    for kind, axes in stages:
        size = 1
        for a in axes:
            size *= dims[AXES.index(a)]
        if kind == "rs":
            piece = next(p for p in range(-(-count // size), count + 1) if count % p == 0)
            owners = count // piece
            out.append((kind, axes, size, owners, piece, (size - 1) * piece))
            stack.append((count, owners))
            count = piece
        elif kind == "bc":
            out.append((kind, axes, size, size, count, size * count))
        else:
            whole, owners = stack.pop()
            out.append((kind, axes, size, owners, count, 0))
            count = whole
    return out


def wait_bytes(ref, sem):
    pltpu.make_async_copy(ref, ref, sem).wait()


def when(condition, body):
    if condition is None:
        body()
    else:
        pl.when(condition)(body)


def both(a, b):
    if a is None or b is None:
        return b if a is None else a
    return jnp.logical_and(a, b)


class Sum:
    def __init__(self, me, pos, dims, strides, stages, count, ar, res, rb, send_sem, recv_sem):
        self.me, self.pos, self.dims, self.strides = me, pos, dims, strides
        self.ar, self.res, self.rb, self.send_sem, self.recv_sem = ar, res, rb, send_sem, recv_sem
        self.plan = plan(dims, stages, count)
        self.drains = []
        self.steps = self.run(count)

    def group(self, axes):
        ids = [AXES.index(a) for a in axes]
        p, base = 0, self.me
        for a in ids:
            p = p * self.dims[a] + self.pos[a]
            base = base - self.pos[a] * self.strides[a]

        def device(q):
            out = base
            for a in reversed(ids):
                out = out + lax.rem(q, self.dims[a]) * self.strides[a]
                q = lax.div(q, self.dims[a])
            return out
        def partner(i):
            to, radix = 0, 1
            for a in reversed(ids):
                d = self.dims[a]
                to = to + lax.rem(self.pos[a] + lax.rem(i, d) + 1, d) * radix
                i, radix = lax.div(i, d), radix * d
            return to

        own = 0
        for a in ids:
            own = own * self.dims[a] + (self.dims[a] - 1)
        return p, device, partner, own

    def others(self, size, own, body):
        if size <= 8:
            for i in range(size):
                if i != own:
                    body(jnp.int32(i), i - (i > own))
            return

        @pl.loop(0, own)
        def _(i):
            body(i, i)

        @pl.loop(own + 1, size)
        def _(i):
            body(i, i - 1)

    def each(self, size, body, first=1):
        if size <= 8:
            for d in range(first, size):
                body(d)
        else:
            pl.loop(first, size)(body)

    def step(self):
        return next(self.steps, False)

    def run(self, count):
        ar, res, rb = self.ar, self.res, self.rb
        first, active, offset, stack = 0, None, 0, []
        for i, (kind, axes, size, owners, piece, slots) in enumerate(self.plan):
            p, device, partner, own = self.group(axes)
            send, recv = self.send_sem.at[i], self.recv_sem.at[i]
            to_of = lambda d: lax.rem(p + d, size)
            if kind == "rs":
                full = owners == size

                def start(i, slot):
                    to = partner(i)
                    copy = pltpu.make_async_remote_copy(
                        src_ref=ar.at[pl.ds(first + to * piece, piece)], dst_ref=rb.at[pl.ds(offset + slot * piece, piece)],
                        send_sem=send, recv_sem=recv, device_id={"nodes": device(to)})
                    when(None if full else to < owners, copy.start)
                when(active, lambda: self.others(size, own, start))
                yield True
                mine = both(active, None if full else p < owners)
                new = first + p * piece
                got = pl.ds(offset, slots)

                def collect():
                    wait_bytes(rb.at[got], recv)
                    total = ar[pl.ds(new, piece)] + jnp.sum(rb[got].reshape(size - 1, piece, 8, 128), axis=0)
                    ar[pl.ds(new, piece)] = total
                    res[pl.ds(new, piece)] = total
                when(mine, collect)
                if full:
                    self.drains.append((active, send, (size - 1) * piece))
                else:
                    self.drains.append((mine, send, (owners - 1) * piece))
                    self.drains.append((both(active, p >= owners), send, owners * piece))
                stack.append((first, active, p, full))
                first, active = new, mine
                offset += slots
            elif kind == "bc":
                mine = pl.ds(first, piece)

                def start(d):
                    to = to_of(d)
                    pltpu.make_async_remote_copy(
                        src_ref=ar.at[mine], dst_ref=rb.at[pl.ds(offset + p * piece, piece)],
                        send_sem=send, recv_sem=recv, device_id={"nodes": device(to)}).start()

                def spread():
                    self.each(size, start)
                    rb[pl.ds(offset + p * piece, piece)] = ar[mine]
                when(active, spread)
                yield True

                def collect():
                    wait_bytes(rb.at[pl.ds(offset, slots - piece)], recv)
                    res[mine] = jnp.sum(rb[pl.ds(offset, slots)].reshape(size, piece, 8, 128), axis=0)
                when(active, collect)
                self.drains.append((active, send, (size - 1) * piece))
                offset += slots
            else:
                mine = pl.ds(first, piece)
                ahead = axes == "zyx" and i + 1 < len(self.plan) and self.plan[i + 1][1] == "c"
                if axes == "c":
                    active = both(active, self.me >= 2)

                def start(to):
                    pl.when(to != p)(pltpu.make_async_remote_copy(
                        src_ref=res.at[mine], dst_ref=res.at[mine],
                        send_sem=send, recv_sem=recv, device_id={"nodes": device(to)}).start)

                def spread():
                    if ahead:
                        pltpu.make_async_remote_copy(
                            src_ref=res.at[mine], dst_ref=res.at[mine],
                            send_sem=send, recv_sem=self.recv_sem.at[i + 1], device_id={"nodes": 1 - self.pos[3]}).start()
                    self.each(size, start, 0)
                when(active, spread)
                yield True
                self.drains.append((active, send, (size - 1 + ahead) * piece))
                first, active, p, full = stack.pop()
                if full:
                    when(active, lambda: wait_bytes(res.at[pl.ds(0, (size - 1) * piece)], recv))
                else:
                    when(both(active, p < owners), lambda: wait_bytes(res.at[pl.ds(0, (owners - 1) * piece)], recv))
                    when(both(active, p >= owners), lambda: wait_bytes(res.at[pl.ds(0, owners * piece)], recv))

    def drain(self):
        for condition, sem, slots in self.drains:
            when(condition, lambda: wait_bytes(self.rb.at[pl.ds(0, slots)], sem))


def kernel(n, xt_hbm, aint_hbm, ahalo_hbm, idx_hbm, w0_hbm, w1t_hbm, gt_hbm, dw1_ref, dw2t_ref, gft,
           xt, aint, ahalo, idx, w0, w1t, gt, st, s, e1t, o1, r1, g0, h0, zpart, d1t, z0t, h1t, g1, zh, z1part, z1t,
           w0t, w1, gtp, ft, e0t, o0, r0, load_sem, halo_send, halo_recv, *sum_refs):
    dims = torus_dims(n)
    strides = tuple(dims[i + 1] * dims[i + 2] * dims[i + 3] if i == 0 else (dims[2] * dims[3], dims[3], 1)[i - 1] for i in range(4))
    me = lax.axis_index("nodes")
    pos = [lax.rem(lax.div(me, stride), d) for stride, d in zip(strides, dims)]
    feats, nodes = xt.shape
    classes, hidden = w1t.shape

    barrier = pltpu.get_barrier_semaphore()

    @pl.loop(1, n)
    def _(i):
        pl.semaphore_signal(barrier, inc=1, device_id={"nodes": lax.rem(me + i, n)})

    loads = [pltpu.make_async_copy(src, dst, load_sem.at[i]) for i, (src, dst) in enumerate([
        (idx_hbm, idx), (xt_hbm, xt), (w1t_hbm, w1t), (gt_hbm, gt), (aint_hbm, aint), (w0_hbm, w0)])]
    for load in loads[:4]:
        load.start()
    for c, k in enumerate(BLOCKS):
        pltpu.make_async_copy(
            ahalo_hbm.at[:, pl.ds(k * SLOTS, SLOTS)], ahalo.at[c // 2, :, pl.ds(c % 2 * SLOTS, SLOTS)], load_sem.at[6]).start()
    for load in loads[4:]:
        load.start()

    ahead = lax.div(pos[2], dims[2] // 2)
    behind = 1 - ahead

    class Halo:
        def __init__(self, which, src, dst, sign):
            self.src, self.dst = src, dst
            self.send, self.recv = halo_send.at[which], [halo_recv.at[2 * which], halo_recv.at[2 * which + 1]]
            self.which, self.sign = which, sign
            self.first, self.second = (behind, ahead) if sign > 0 else (ahead, behind)

        def start(self):
            for c in ISSUE:
                o = OFFSETS[BLOCKS[c]]
                pltpu.make_async_remote_copy(
                    src_ref=self.src.at[c // 2, c % 2], dst_ref=self.dst.at[c // 2, c % 2], send_sem=self.send, recv_sem=self.recv[c // 2],
                    device_id={"nodes": lax.rem(me + self.sign * o + n, n)}).start()

        def wait_recv(self, half):
            wait_bytes(self.dst.at[half], halo_recv.at[2 * self.which + half])

        def wait_send(self):
            wait_bytes(self.src, self.send)

    halo_x = Halo(0, g0, h0, 1)
    halo_d1 = Halo(1, o1, r1, -1)
    halo_z = Halo(2, g1, zh, 1)
    halo_d0 = Halo(3, o0, r0, -1)
    sums = []
    for i, (_, _, _, stages) in enumerate(SUMS):
        refs = sum_refs[5 * i:5 * i + 5]
        sums.append(Sum(me, pos, dims, strides, stages, refs[0].shape[0], *refs))

    def put(ref, value):
        for c in range(4):
            ref[c // 2, c % 2] = value[:, c * SLOTS:(c + 1) * SLOTS].astype(BF)

    def take(ref, half):
        return jnp.concatenate([ref[half, 0], ref[half, 1]], axis=1)

    def outward(rows):
        return jnp.concatenate([dot(rows, ahalo[0]), dot(rows, ahalo[1])], axis=1)

    def half_rows(half):
        return s[pl.ds(pl.multiple_of(half * 2 * SLOTS, 2 * SLOTS), 2 * SLOTS)]

    loads[0].wait()
    sub = lax.broadcasted_iota(jnp.int32, (nodes, SLOTS), 0)
    for c, k in enumerate(BLOCKS):
        row = jnp.broadcast_to(idx[k:k + 1, :], (nodes, SLOTS))
        st[:, c * SLOTS:(c + 1) * SLOTS] = jnp.where(row == sub, 1.0, 0.0).astype(BF)

    loads[1].wait()
    put(g0, dot(xt[...], st[...]))
    loads[2].wait()
    loads[3].wait()
    w1[...] = jnp.concatenate([w1t[...].astype(F32), jnp.zeros((128 - classes, hidden), F32)], axis=0).T.astype(BF)
    gtp[...] = jnp.concatenate([gt[...].astype(F32), jnp.zeros((128 - classes, nodes), F32)], axis=0).astype(BF)
    e1t[...] = dot(w1[...], gtp[...]).astype(BF)
    wait_bytes(ahalo, load_sem.at[6])
    put(o1, outward(e1t[...]))

    pl.semaphore_wait(barrier, n - 1)
    halo_x.start()

    loads[4].wait()
    loads[5].wait()
    zpart[...] = dot_nt(xt[...], aint[...])
    halo_d1.start()
    w0t[...] = w0[...].astype(F32).T.astype(BF)
    lane = lax.broadcasted_iota(jnp.int32, (SLOTS, SLOTS), 1)
    for c, k in enumerate(BLOCKS):
        col = jnp.broadcast_to(idx[k:k + 1, :], (SLOTS, SLOTS)).T
        for b in range(nodes // SLOTS):
            s[c * SLOTS:(c + 1) * SLOTS, b * SLOTS:(b + 1) * SLOTS] = jnp.where(col == lane + b * SLOTS, 1.0, 0.0).astype(BF)
    d1t[...] = dot(e1t[...], aint[...])

    def hidden_of(zt):
        return jnp.maximum(dot(w0t[...], zt), 0.0).astype(BF)

    halo_x.wait_recv(halo_x.first)
    zpart[...] = zpart[...] + dot_nt(take(h0, halo_x.first), ahalo[halo_x.first])
    halo_x.wait_recv(halo_x.second)
    z0t[...] = (zpart[...] + dot_nt(take(h0, halo_x.second), ahalo[halo_x.second])).astype(BF)
    put(g1, dot(z0t[...], st[...]))
    halo_z.start()
    h1t[...] = hidden_of(z0t[...])
    z1part[...] = dot_nt(h1t[...], aint[...])

    halo_d1.wait_recv(halo_d1.first)
    d1t[...] = d1t[...] + dot(take(r1, halo_d1.first), half_rows(halo_d1.first))
    halo_d1.wait_recv(halo_d1.second)
    d1 = d1t[...] + dot(take(r1, halo_d1.second), half_rows(halo_d1.second))
    ft[...] = jnp.where(h1t[...] > 0, d1, 0.0).astype(BF)

    def to_chunks(which, value):
        groups = value.shape[0] // 8
        for (weight, lo, hi, _), total in zip(SUMS, sums):
            if weight == which:
                for k in range(lo, hi):
                    total.ar[(k - lo) * groups:(k - lo + 1) * groups] = value[:, k * 128:(k + 1) * 128].reshape(groups, 8, 128)

    def step(i):
        weight, lo, hi, _ = SUMS[i]
        if sums[i].step():
            return
        left.remove(i)
        out_ref, rows = (dw1_ref, feats) if weight == 1 else (dw2t_ref, classes)
        groups = sums[i].res.shape[0] // (hi - lo)
        for k in range(lo, hi):
            out_ref[:, k * 128:(k + 1) * 128] = sums[i].res[(k - lo) * groups:(k - lo + 1) * groups].reshape(groups * 8, 128)[0:rows]

    left = list(range(len(SUMS)))
    for event in ORDER:
        if event == "W":
            to_chunks(1, dot_nt(z0t[...], ft[...]))
        elif event == "E":
            e0t[...] = dot(w0[...], ft[...]).astype(BF)
            put(o0, outward(e0t[...]))
            halo_d0.start()
        elif event == "Z":
            halo_z.wait_recv(halo_z.first)
            z1part[...] = z1part[...] + dot_nt(hidden_of(take(zh, halo_z.first)), ahalo[halo_z.first])
            halo_z.wait_recv(halo_z.second)
            z1t[...] = (z1part[...] + dot_nt(hidden_of(take(zh, halo_z.second)), ahalo[halo_z.second])).astype(BF)
            padded = -(-classes // 8) * 8
            to_chunks(2, dot_nt(gtp[...], z1t[...])[0:padded])
        elif event == "g":
            gft[...] = dot(e0t[...], aint[...])
        elif event == "d":
            for half in range(2):
                halo_d0.wait_recv(half)
                gft[...] = gft[...] + dot(take(r0, half), half_rows(half))
        else:
            step("abcABC".index(event))
    assert not left
    for halo in (halo_x, halo_d1, halo_z, halo_d0):
        halo.wait_send()
    for total in sums:
        total.drain()


def write_out(a, b, c, x, y, z, sem):
    copies = [pltpu.make_async_copy(src, dst, sem.at[i]) for i, (src, dst) in enumerate([(a, x), (b, y), (c, z)])]
    for copy in copies:
        copy.start()
    for copy in copies:
        copy.wait()


def solution(mesh):
    n = mesh.shape["nodes"]
    dims = torus_dims(n)
    row_spec = P(("graph", "nodes"), None)
    replicated = P(None, None)
    part_spec = P("graph", None)

    def device_step(node_feats, a_int, a_halo, send_idx, w_first, w_second, grad_out):
        nodes, feats = node_feats.shape
        hidden, classes = w_second.shape
        slots = a_halo.shape[1]
        v = pltpu.VMEM
        dma = pltpu.SemaphoreType.DMA
        groups = {1: feats // 8, 2: -(-classes // 8)}
        sum_refs = []
        for weight, lo, hi, stages in SUMS:
            count = groups[weight] * (hi - lo)
            received = sum(p[5] for p in plan(dims, stages, count))
            sum_refs += [v((count, 8, 128), F32), v((count, 8, 128), F32), v((received, 8, 128), F32), dma((len(stages),)), dma((len(stages),))]
        outs = pl.pallas_call(
            functools.partial(kernel, n),
            out_shape=(v((feats, hidden), F32), v((classes, hidden), F32), v((feats, nodes), F32)),
            in_specs=[ANY] * 7,
            out_specs=[VMEM] * 3,
            scratch_shapes=[
                v((feats, nodes), BF),
                v((nodes, nodes), BF),
                v((2, nodes, slots // 2), BF),
                v((4, SLOTS), jnp.int32),
                v((feats, hidden), BF),
                v((classes, hidden), BF),
                v((classes, nodes), BF),
                v((nodes, slots), BF),
                v((slots, nodes), BF),
                v((hidden, nodes), BF),
                v((2, 2, hidden, SLOTS), BF),
                v((2, 2, hidden, SLOTS), BF),
                v((2, 2, feats, SLOTS), BF),
                v((2, 2, feats, SLOTS), BF),
                v((feats, nodes), F32),
                v((hidden, nodes), F32),
                v((feats, nodes), BF),
                v((hidden, nodes), BF),
                v((2, 2, feats, SLOTS), BF),
                v((2, 2, feats, SLOTS), BF),
                v((hidden, nodes), F32),
                v((hidden, nodes), BF),
                v((hidden, feats), BF),
                v((hidden, 128), BF),
                v((128, nodes), BF),
                v((hidden, nodes), BF),
                v((feats, nodes), BF),
                v((2, 2, feats, SLOTS), BF),
                v((2, 2, feats, SLOTS), BF),
                dma((7,)), dma((4,)), dma((8,)),
                *sum_refs,
            ],
            compiler_params=pltpu.CompilerParams(collective_id=0, has_side_effects=True, vmem_limit_bytes=40 << 20),
        )(*[pltpu.with_memory_space_constraint(a, pltpu.HBM) for a in
            (node_feats.T, a_int, a_halo, send_idx, w_first, w_second.T, grad_out.T)])
        dw1, dw2t, gft = pl.pallas_call(
            write_out,
            out_shape=tuple(jax.ShapeDtypeStruct(o.shape, F32) for o in outs),
            in_specs=[VMEM] * 3,
            out_specs=[ANY] * 3,
            scratch_shapes=[dma((3,))],
            compiler_params=pltpu.CompilerParams(vmem_limit_bytes=1 << 20),
        )(*outs)
        return dw1, dw2t.T, gft.T

    return jax.shard_map(device_step, mesh=mesh, in_specs=(row_spec, row_spec, row_spec, row_spec, replicated, replicated, row_spec), out_specs=(part_spec, part_spec, row_spec), check_vma=False)
```

```python
import functools

import jax
import jax.numpy as jnp
from jax import lax
from jax.experimental import pallas as pl
from jax.experimental.pallas import tpu as pltpu
from jax.sharding import PartitionSpec as P

BF = jnp.bfloat16
F32 = jnp.float32
OFFSETS = (1, -1, 2, -2)
BLOCKS = (0, 2, 1, 3)
ISSUE = (0, 2, 1, 3)
SLOTS = 128
ANY = pl.BlockSpec(memory_space=pl.ANY)
VMEM = pl.BlockSpec(memory_space=pltpu.VMEM)
FULL = (("rs", "c"), ("rs", "zyx"), ("ag", "zyx"), ("ag", "c"))
PLANE = (("rs", "zy"), ("bc", "xc"), ("ag", "zy"))
SUMS = (
    (1, 0, 4, FULL),
    (2, 0, 4, PLANE),
)
ORDER = "WaEZbagbabdaab"
AXES = "zyxc"


def torus_dims(n):
    return {128: (4, 4, 4, 2), 16: (2, 2, 2, 2)}[n]


def dot(a, b):
    return jnp.dot(a, b, preferred_element_type=F32)


def dot_nt(a, b):
    return lax.dot_general(a, b, (((1,), (1,)), ((), ())), preferred_element_type=F32)


def plan(dims, stages, count):
    out, stack = [], []
    for kind, axes in stages:
        size = 1
        for a in axes:
            size *= dims[AXES.index(a)]
        if kind == "rs":
            piece = next(p for p in range(-(-count // size), count + 1) if count % p == 0)
            owners = count // piece
            out.append((kind, axes, size, owners, piece, (size - 1) * piece))
            stack.append((count, owners))
            count = piece
        elif kind == "bc":
            out.append((kind, axes, size, size, count, size * count))
        else:
            whole, owners = stack.pop()
            out.append((kind, axes, size, owners, count, 0))
            count = whole
    return out


def wait_bytes(ref, sem):
    pltpu.make_async_copy(ref, ref, sem).wait()


def when(condition, body):
    if condition is None:
        body()
    else:
        pl.when(condition)(body)


def both(a, b):
    if a is None or b is None:
        return b if a is None else a
    return jnp.logical_and(a, b)


class Sum:
    def __init__(self, me, pos, dims, strides, stages, count, ar, res, rb, send_sem, recv_sem):
        self.me, self.pos, self.dims, self.strides = me, pos, dims, strides
        self.ar, self.res, self.rb, self.send_sem, self.recv_sem = ar, res, rb, send_sem, recv_sem
        self.plan = plan(dims, stages, count)
        self.drains = []
        self.steps = self.run(count)

    def group(self, axes):
        ids = [AXES.index(a) for a in axes]
        p, base = 0, self.me
        for a in ids:
            p = p * self.dims[a] + self.pos[a]
            base = base - self.pos[a] * self.strides[a]

        def device(q):
            out = base
            for a in reversed(ids):
                out = out + lax.rem(q, self.dims[a]) * self.strides[a]
                q = lax.div(q, self.dims[a])
            return out
        def partner(i):
            to, radix = 0, 1
            for a in reversed(ids):
                d = self.dims[a]
                to = to + lax.rem(self.pos[a] + lax.rem(i, d) + 1, d) * radix
                i, radix = lax.div(i, d), radix * d
            return to

        own = 0
        for a in ids:
            own = own * self.dims[a] + (self.dims[a] - 1)
        return p, device, partner, own

    def others(self, size, own, body):
        if size <= 8:
            for i in range(size):
                if i != own:
                    body(jnp.int32(i), i - (i > own))
            return

        @pl.loop(0, own)
        def _(i):
            body(i, i)

        @pl.loop(own + 1, size)
        def _(i):
            body(i, i - 1)

    def each(self, size, body, first=1):
        if size <= 8:
            for d in range(first, size):
                body(d)
        else:
            pl.loop(first, size)(body)

    def step(self):
        return next(self.steps, False)

    def run(self, count):
        ar, res, rb = self.ar, self.res, self.rb
        first, active, offset, stack = 0, None, 0, []
        for i, (kind, axes, size, owners, piece, slots) in enumerate(self.plan):
            p, device, partner, own = self.group(axes)
            send, recv = self.send_sem.at[i], self.recv_sem.at[i]
            to_of = lambda d: lax.rem(p + d, size)
            if kind == "rs":
                full = owners == size

                def start(i, slot):
                    to = partner(i)
                    copy = pltpu.make_async_remote_copy(
                        src_ref=ar.at[pl.ds(first + to * piece, piece)], dst_ref=rb.at[pl.ds(offset + slot * piece, piece)],
                        send_sem=send, recv_sem=recv, device_id={"nodes": device(to)})
                    when(None if full else to < owners, copy.start)
                when(active, lambda: self.others(size, own, start))
                yield True
                mine = both(active, None if full else p < owners)
                new = first + p * piece
                got = pl.ds(offset, slots)

                def collect():
                    wait_bytes(rb.at[got], recv)
                    total = ar[pl.ds(new, piece)] + jnp.sum(rb[got].reshape(size - 1, piece, 8, 128), axis=0)
                    ar[pl.ds(new, piece)] = total
                    res[pl.ds(new, piece)] = total
                when(mine, collect)
                if full:
                    self.drains.append((active, send, (size - 1) * piece))
                else:
                    self.drains.append((mine, send, (owners - 1) * piece))
                    self.drains.append((both(active, p >= owners), send, owners * piece))
                stack.append((first, active, p, full))
                first, active = new, mine
                offset += slots
            elif kind == "bc":
                mine = pl.ds(first, piece)

                def start(d):
                    to = to_of(d)
                    pltpu.make_async_remote_copy(
                        src_ref=ar.at[mine], dst_ref=rb.at[pl.ds(offset + p * piece, piece)],
                        send_sem=send, recv_sem=recv, device_id={"nodes": device(to)}).start()

                def spread():
                    self.each(size, start)
                    rb[pl.ds(offset + p * piece, piece)] = ar[mine]
                when(active, spread)
                yield True

                def collect():
                    wait_bytes(rb.at[pl.ds(offset, slots - piece)], recv)
                    res[mine] = jnp.sum(rb[pl.ds(offset, slots)].reshape(size, piece, 8, 128), axis=0)
                when(active, collect)
                self.drains.append((active, send, (size - 1) * piece))
                offset += slots
            else:
                mine = pl.ds(first, piece)
                ahead = axes == "zyx" and i + 1 < len(self.plan) and self.plan[i + 1][1] == "c"
                if axes == "c":
                    active = both(active, self.me >= 2)

                def start(to):
                    pl.when(to != p)(pltpu.make_async_remote_copy(
                        src_ref=res.at[mine], dst_ref=res.at[mine],
                        send_sem=send, recv_sem=recv, device_id={"nodes": device(to)}).start)

                def spread():
                    if ahead:
                        pltpu.make_async_remote_copy(
                            src_ref=res.at[mine], dst_ref=res.at[mine],
                            send_sem=send, recv_sem=self.recv_sem.at[i + 1], device_id={"nodes": 1 - self.pos[3]}).start()
                    self.each(size, start, 0)
                when(active, spread)
                yield True
                self.drains.append((active, send, (size - 1 + ahead) * piece))
                first, active, p, full = stack.pop()
                if full:
                    when(active, lambda: wait_bytes(res.at[pl.ds(0, (size - 1) * piece)], recv))
                else:
                    when(both(active, p < owners), lambda: wait_bytes(res.at[pl.ds(0, (owners - 1) * piece)], recv))
                    when(both(active, p >= owners), lambda: wait_bytes(res.at[pl.ds(0, owners * piece)], recv))

    def drain(self):
        for condition, sem, slots in self.drains:
            when(condition, lambda: wait_bytes(self.rb.at[pl.ds(0, slots)], sem))


def kernel(n, xt_hbm, aint_hbm, ahalo_hbm, idx_hbm, w0_hbm, w1t_hbm, gt_hbm, dw1_ref, dw2t_ref, gft,
           xt, aint, ahalo, idx, w0, w1t, gt, st, s, e1t, o1, r1, g0, h0, zpart, d1t, z0t, h1t, g1, zh, z1part, z1t,
           w0t, w1, gtp, ft, e0t, o0, r0, load_sem, halo_send, halo_recv, *sum_refs):
    dims = torus_dims(n)
    strides = tuple(dims[i + 1] * dims[i + 2] * dims[i + 3] if i == 0 else (dims[2] * dims[3], dims[3], 1)[i - 1] for i in range(4))
    me = lax.axis_index("nodes")
    pos = [lax.rem(lax.div(me, stride), d) for stride, d in zip(strides, dims)]
    feats, nodes = xt.shape
    classes, hidden = w1t.shape

    barrier = pltpu.get_barrier_semaphore()

    def greet(i):
        pl.semaphore_signal(barrier, inc=1, device_id={"nodes": lax.rem(me + i, n)})

    for i in (1, 2, n - 2, n - 1):
        greet(i)

    loads = [pltpu.make_async_copy(src, dst, load_sem.at[i]) for i, (src, dst) in enumerate([
        (idx_hbm, idx), (xt_hbm, xt), (w1t_hbm, w1t), (gt_hbm, gt), (aint_hbm, aint), (w0_hbm, w0)])]
    for load in loads[:4]:
        load.start()
    for c, k in enumerate(BLOCKS):
        pltpu.make_async_copy(
            ahalo_hbm.at[:, pl.ds(k * SLOTS, SLOTS)], ahalo.at[c // 2, :, pl.ds(c % 2 * SLOTS, SLOTS)], load_sem.at[6]).start()
    for load in loads[4:]:
        load.start()
    pl.loop(3, n - 2)(greet)

    ahead = lax.div(pos[2], dims[2] // 2)
    behind = 1 - ahead

    class Halo:
        def __init__(self, which, src, dst, sign):
            self.src, self.dst = src, dst
            self.send, self.recv = halo_send.at[which], [halo_recv.at[2 * which], halo_recv.at[2 * which + 1]]
            self.which, self.sign = which, sign
            self.first, self.second = (behind, ahead) if sign > 0 else (ahead, behind)

        def start(self):
            for c in ISSUE:
                o = OFFSETS[BLOCKS[c]]
                pltpu.make_async_remote_copy(
                    src_ref=self.src.at[c // 2, c % 2], dst_ref=self.dst.at[c // 2, c % 2], send_sem=self.send, recv_sem=self.recv[c // 2],
                    device_id={"nodes": lax.rem(me + self.sign * o + n, n)}).start()

        def wait_recv(self, half):
            wait_bytes(self.dst.at[half], halo_recv.at[2 * self.which + half])

        def wait_send(self):
            wait_bytes(self.src, self.send)

    halo_x = Halo(0, g0, h0, 1)
    halo_d1 = Halo(1, o1, r1, -1)
    halo_z = Halo(2, g1, zh, 1)
    halo_d0 = Halo(3, o0, r0, -1)
    sums = []
    for i, (_, _, _, stages) in enumerate(SUMS):
        refs = sum_refs[5 * i:5 * i + 5]
        sums.append(Sum(me, pos, dims, strides, stages, refs[0].shape[0], *refs))

    def put(ref, value):
        for c in range(4):
            ref[c // 2, c % 2] = value[:, c * SLOTS:(c + 1) * SLOTS].astype(BF)

    def take(ref, half):
        return jnp.concatenate([ref[half, 0], ref[half, 1]], axis=1)

    def outward(rows):
        return jnp.concatenate([dot(rows, ahalo[0]), dot(rows, ahalo[1])], axis=1)

    def half_rows(half):
        return s[pl.ds(pl.multiple_of(half * 2 * SLOTS, 2 * SLOTS), 2 * SLOTS)]

    loads[0].wait()
    sub = lax.broadcasted_iota(jnp.int32, (nodes, SLOTS), 0)
    for c, k in enumerate(BLOCKS):
        row = jnp.broadcast_to(idx[k:k + 1, :], (nodes, SLOTS))
        st[:, c * SLOTS:(c + 1) * SLOTS] = jnp.where(row == sub, 1.0, 0.0).astype(BF)

    loads[1].wait()
    put(g0, dot(xt[...], st[...]))
    loads[2].wait()
    loads[3].wait()
    w1[...] = jnp.concatenate([w1t[...].astype(F32), jnp.zeros((128 - classes, hidden), F32)], axis=0).T.astype(BF)
    gtp[...] = jnp.concatenate([gt[...].astype(F32), jnp.zeros((128 - classes, nodes), F32)], axis=0).astype(BF)
    e1t[...] = dot(w1[...], gtp[...]).astype(BF)
    wait_bytes(ahalo, load_sem.at[6])
    put(o1, outward(e1t[...]))

    pl.semaphore_wait(barrier, n - 1)
    halo_x.start()

    loads[4].wait()
    loads[5].wait()
    zpart[...] = dot_nt(xt[...], aint[...])
    halo_d1.start()
    w0t[...] = w0[...].astype(F32).T.astype(BF)
    lane = lax.broadcasted_iota(jnp.int32, (SLOTS, SLOTS), 1)
    for c, k in enumerate(BLOCKS):
        col = jnp.broadcast_to(idx[k:k + 1, :], (SLOTS, SLOTS)).T
        for b in range(nodes // SLOTS):
            s[c * SLOTS:(c + 1) * SLOTS, b * SLOTS:(b + 1) * SLOTS] = jnp.where(col == lane + b * SLOTS, 1.0, 0.0).astype(BF)
    d1t[...] = dot(e1t[...], aint[...])

    def hidden_of(zt):
        return jnp.maximum(dot(w0t[...], zt), 0.0).astype(BF)

    halo_x.wait_recv(halo_x.first)
    zpart[...] = zpart[...] + dot_nt(take(h0, halo_x.first), ahalo[halo_x.first])
    halo_x.wait_recv(halo_x.second)
    z0t[...] = (zpart[...] + dot_nt(take(h0, halo_x.second), ahalo[halo_x.second])).astype(BF)
    put(g1, dot(z0t[...], st[...]))
    halo_z.start()
    h1t[...] = hidden_of(z0t[...])
    z1part[...] = dot_nt(h1t[...], aint[...])

    halo_d1.wait_recv(halo_d1.first)
    d1t[...] = d1t[...] + dot(take(r1, halo_d1.first), half_rows(halo_d1.first))
    halo_d1.wait_recv(halo_d1.second)
    d1 = d1t[...] + dot(take(r1, halo_d1.second), half_rows(halo_d1.second))
    ft[...] = jnp.where(h1t[...] > 0, d1, 0.0).astype(BF)

    def to_chunks(which, value):
        groups = value.shape[0] // 8
        for (weight, lo, hi, _), total in zip(SUMS, sums):
            if weight == which:
                for k in range(lo, hi):
                    total.ar[(k - lo) * groups:(k - lo + 1) * groups] = value[:, k * 128:(k + 1) * 128].reshape(groups, 8, 128)

    def step(i):
        weight, lo, hi, _ = SUMS[i]
        if sums[i].step():
            return
        left.remove(i)
        out_ref, rows = (dw1_ref, feats) if weight == 1 else (dw2t_ref, classes)
        groups = sums[i].res.shape[0] // (hi - lo)
        for k in range(lo, hi):
            out_ref[:, k * 128:(k + 1) * 128] = sums[i].res[(k - lo) * groups:(k - lo + 1) * groups].reshape(groups * 8, 128)[0:rows]

    left = list(range(len(SUMS)))
    for event in ORDER:
        if event == "W":
            to_chunks(1, dot_nt(z0t[...], ft[...]))
        elif event == "E":
            e0t[...] = dot(w0[...], ft[...]).astype(BF)
            put(o0, outward(e0t[...]))
            halo_d0.start()
        elif event == "Z":
            halo_z.wait_recv(halo_z.first)
            z1part[...] = z1part[...] + dot_nt(hidden_of(take(zh, halo_z.first)), ahalo[halo_z.first])
            halo_z.wait_recv(halo_z.second)
            z1t[...] = (z1part[...] + dot_nt(hidden_of(take(zh, halo_z.second)), ahalo[halo_z.second])).astype(BF)
            padded = -(-classes // 8) * 8
            to_chunks(2, dot_nt(gtp[...], z1t[...])[0:padded])
        elif event == "g":
            gft[...] = dot(e0t[...], aint[...])
        elif event == "d":
            for half in range(2):
                halo_d0.wait_recv(half)
                gft[...] = gft[...] + dot(take(r0, half), half_rows(half))
        else:
            step("abcABC".index(event))
    assert not left
    for halo in (halo_x, halo_d1, halo_z, halo_d0):
        halo.wait_send()
    for total in sums:
        total.drain()


def write_out(a, b, c, x, y, z, sem):
    copies = [pltpu.make_async_copy(src, dst, sem.at[i]) for i, (src, dst) in enumerate([(a, x), (b, y), (c, z)])]
    for copy in copies:
        copy.start()
    for copy in copies:
        copy.wait()


def solution(mesh):
    n = mesh.shape["nodes"]
    dims = torus_dims(n)
    row_spec = P(("graph", "nodes"), None)
    replicated = P(None, None)
    part_spec = P("graph", None)

    def device_step(node_feats, a_int, a_halo, send_idx, w_first, w_second, grad_out):
        nodes, feats = node_feats.shape
        hidden, classes = w_second.shape
        slots = a_halo.shape[1]
        v = pltpu.VMEM
        dma = pltpu.SemaphoreType.DMA
        groups = {1: feats // 8, 2: -(-classes // 8)}
        sum_refs = []
        for weight, lo, hi, stages in SUMS:
            count = groups[weight] * (hi - lo)
            received = sum(p[5] for p in plan(dims, stages, count))
            sum_refs += [v((count, 8, 128), F32), v((count, 8, 128), F32), v((received, 8, 128), F32), dma((len(stages),)), dma((len(stages),))]
        outs = pl.pallas_call(
            functools.partial(kernel, n),
            out_shape=(v((feats, hidden), F32), v((classes, hidden), F32), v((feats, nodes), F32)),
            in_specs=[ANY] * 7,
            out_specs=[VMEM] * 3,
            scratch_shapes=[
                v((feats, nodes), BF),
                v((nodes, nodes), BF),
                v((2, nodes, slots // 2), BF),
                v((4, SLOTS), jnp.int32),
                v((feats, hidden), BF),
                v((classes, hidden), BF),
                v((classes, nodes), BF),
                v((nodes, slots), BF),
                v((slots, nodes), BF),
                v((hidden, nodes), BF),
                v((2, 2, hidden, SLOTS), BF),
                v((2, 2, hidden, SLOTS), BF),
                v((2, 2, feats, SLOTS), BF),
                v((2, 2, feats, SLOTS), BF),
                v((feats, nodes), F32),
                v((hidden, nodes), F32),
                v((feats, nodes), BF),
                v((hidden, nodes), BF),
                v((2, 2, feats, SLOTS), BF),
                v((2, 2, feats, SLOTS), BF),
                v((hidden, nodes), F32),
                v((hidden, nodes), BF),
                v((hidden, feats), BF),
                v((hidden, 128), BF),
                v((128, nodes), BF),
                v((hidden, nodes), BF),
                v((feats, nodes), BF),
                v((2, 2, feats, SLOTS), BF),
                v((2, 2, feats, SLOTS), BF),
                dma((7,)), dma((4,)), dma((8,)),
                *sum_refs,
            ],
            compiler_params=pltpu.CompilerParams(collective_id=0, has_side_effects=True, vmem_limit_bytes=40 << 20),
        )(*[pltpu.with_memory_space_constraint(a, pltpu.HBM) for a in
            (node_feats.T, a_int, a_halo, send_idx, w_first, w_second.T, grad_out.T)])
        dw1, dw2t, gft = pl.pallas_call(
            write_out,
            out_shape=tuple(jax.ShapeDtypeStruct(o.shape, F32) for o in outs),
            in_specs=[VMEM] * 3,
            out_specs=[ANY] * 3,
            scratch_shapes=[dma((3,))],
            compiler_params=pltpu.CompilerParams(vmem_limit_bytes=1 << 20),
        )(*outs)
        return dw1, dw2t.T, gft.T

    return jax.shard_map(device_step, mesh=mesh, in_specs=(row_spec, row_spec, row_spec, row_spec, replicated, replicated, row_spec), out_specs=(part_spec, part_spec, row_spec), check_vma=False)
```

```python
import functools

import jax
import jax.numpy as jnp
from jax import lax
from jax.experimental import pallas as pl
from jax.experimental.pallas import tpu as pltpu
from jax.sharding import PartitionSpec as P

BF = jnp.bfloat16
F32 = jnp.float32
OFFSETS = (1, -1, 2, -2)
BLOCKS = (0, 2, 1, 3)
ISSUE = (0, 2, 1, 3)
SLOTS = 128
ANY = pl.BlockSpec(memory_space=pl.ANY)
VMEM = pl.BlockSpec(memory_space=pltpu.VMEM)
FULL = (("rs", "c"), ("rs", "zyx"), ("ag", "zyx"), ("ag", "c"))
PLANE = (("rs", "zy"), ("bc", "xc"), ("ag", "zy"))
SUMS = (
    (1, 0, 4, FULL),
    (2, 0, 4, PLANE),
)
ORDER = "WaEZbagbabdaab"
AXES = "zyxc"


def torus_dims(n):
    return {128: (4, 4, 4, 2), 16: (2, 2, 2, 2)}[n]


def dot(a, b):
    return jnp.dot(a, b, preferred_element_type=F32)


def dot_nt(a, b):
    return lax.dot_general(a, b, (((1,), (1,)), ((), ())), preferred_element_type=F32)


def plan(dims, stages, count):
    out, stack = [], []
    for kind, axes in stages:
        size = 1
        for a in axes:
            size *= dims[AXES.index(a)]
        if kind == "rs":
            piece = next(p for p in range(-(-count // size), count + 1) if count % p == 0)
            owners = count // piece
            out.append((kind, axes, size, owners, piece, (size - 1) * piece))
            stack.append((count, owners))
            count = piece
        elif kind == "bc":
            out.append((kind, axes, size, size, count, size * count))
        else:
            whole, owners = stack.pop()
            out.append((kind, axes, size, owners, count, 0))
            count = whole
    return out


def wait_bytes(ref, sem):
    pltpu.make_async_copy(ref, ref, sem).wait()


def when(condition, body):
    if condition is None:
        body()
    else:
        pl.when(condition)(body)


def both(a, b):
    if a is None or b is None:
        return b if a is None else a
    return jnp.logical_and(a, b)


class Sum:
    def __init__(self, me, pos, dims, strides, stages, count, ar, res, rb, send_sem, recv_sem):
        self.me, self.pos, self.dims, self.strides = me, pos, dims, strides
        self.ar, self.res, self.rb, self.send_sem, self.recv_sem = ar, res, rb, send_sem, recv_sem
        self.plan = plan(dims, stages, count)
        self.drains = []
        self.steps = self.run(count)

    def group(self, axes):
        ids = [AXES.index(a) for a in axes]
        p, base = 0, self.me
        for a in ids:
            p = p * self.dims[a] + self.pos[a]
            base = base - self.pos[a] * self.strides[a]

        def device(q):
            out = base
            for a in reversed(ids):
                out = out + lax.rem(q, self.dims[a]) * self.strides[a]
                q = lax.div(q, self.dims[a])
            return out
        def partner(i):
            to, radix = 0, 1
            for a in reversed(ids):
                d = self.dims[a]
                to = to + lax.rem(self.pos[a] + lax.rem(i, d) + 1, d) * radix
                i, radix = lax.div(i, d), radix * d
            return to

        own = 0
        for a in ids:
            own = own * self.dims[a] + (self.dims[a] - 1)
        return p, device, partner, own

    def others(self, size, own, body):
        if size <= 8:
            for i in range(size):
                if i != own:
                    body(jnp.int32(i), i - (i > own))
            return

        @pl.loop(0, own)
        def _(i):
            body(i, i)

        @pl.loop(own + 1, size)
        def _(i):
            body(i, i - 1)

    def each(self, size, body, first=1):
        if size <= 8:
            for d in range(first, size):
                body(d)
        else:
            pl.loop(first, size)(body)

    def step(self):
        return next(self.steps, False)

    def run(self, count):
        ar, res, rb = self.ar, self.res, self.rb
        first, active, offset, stack = 0, None, 0, []
        for i, (kind, axes, size, owners, piece, slots) in enumerate(self.plan):
            p, device, partner, own = self.group(axes)
            send, recv = self.send_sem.at[i], self.recv_sem.at[i]
            to_of = lambda d: lax.rem(p + d, size)
            if kind == "rs":
                full = owners == size

                def start(i, slot):
                    to = partner(i)
                    copy = pltpu.make_async_remote_copy(
                        src_ref=ar.at[pl.ds(first + to * piece, piece)], dst_ref=rb.at[pl.ds(offset + slot * piece, piece)],
                        send_sem=send, recv_sem=recv, device_id={"nodes": device(to)})
                    when(None if full else to < owners, copy.start)
                when(active, lambda: self.others(size, own, start))
                yield True
                mine = both(active, None if full else p < owners)
                new = first + p * piece
                got = pl.ds(offset, slots)

                def collect():
                    wait_bytes(rb.at[got], recv)
                    total = ar[pl.ds(new, piece)] + jnp.sum(rb[got].reshape(size - 1, piece, 8, 128), axis=0)
                    ar[pl.ds(new, piece)] = total
                    res[pl.ds(new, piece)] = total
                when(mine, collect)
                if full:
                    self.drains.append((active, send, (size - 1) * piece))
                else:
                    self.drains.append((mine, send, (owners - 1) * piece))
                    self.drains.append((both(active, p >= owners), send, owners * piece))
                stack.append((first, active, p, full))
                first, active = new, mine
                offset += slots
            elif kind == "bc":
                mine = pl.ds(first, piece)

                def start(d):
                    to = to_of(d)
                    pltpu.make_async_remote_copy(
                        src_ref=ar.at[mine], dst_ref=rb.at[pl.ds(offset + p * piece, piece)],
                        send_sem=send, recv_sem=recv, device_id={"nodes": device(to)}).start()

                def spread():
                    self.each(size, start)
                    rb[pl.ds(offset + p * piece, piece)] = ar[mine]
                when(active, spread)
                yield True

                def collect():
                    wait_bytes(rb.at[pl.ds(offset, slots - piece)], recv)
                    res[mine] = jnp.sum(rb[pl.ds(offset, slots)].reshape(size, piece, 8, 128), axis=0)
                when(active, collect)
                self.drains.append((active, send, (size - 1) * piece))
                offset += slots
            else:
                mine = pl.ds(first, piece)
                ahead = axes == "zyx" and i + 1 < len(self.plan) and self.plan[i + 1][1] == "c"
                if axes == "c":
                    active = both(active, self.me >= 2)

                def start(to):
                    pl.when(to != p)(pltpu.make_async_remote_copy(
                        src_ref=res.at[mine], dst_ref=res.at[mine],
                        send_sem=send, recv_sem=recv, device_id={"nodes": device(to)}).start)

                def spread():
                    if ahead:
                        pltpu.make_async_remote_copy(
                            src_ref=res.at[mine], dst_ref=res.at[mine],
                            send_sem=send, recv_sem=self.recv_sem.at[i + 1], device_id={"nodes": 1 - self.pos[3]}).start()
                    self.each(size, start, 0)
                when(active, spread)
                yield True
                self.drains.append((active, send, (size - 1 + ahead) * piece))
                first, active, p, full = stack.pop()
                if full:
                    when(active, lambda: wait_bytes(res.at[pl.ds(0, (size - 1) * piece)], recv))
                else:
                    when(both(active, p < owners), lambda: wait_bytes(res.at[pl.ds(0, (owners - 1) * piece)], recv))
                    when(both(active, p >= owners), lambda: wait_bytes(res.at[pl.ds(0, owners * piece)], recv))

    def drain(self):
        for condition, sem, slots in self.drains:
            when(condition, lambda: wait_bytes(self.rb.at[pl.ds(0, slots)], sem))


def kernel(n, xt_hbm, aint_hbm, ahalo_hbm, idx_hbm, w0_hbm, w1t_hbm, gt_hbm, dw1_ref, dw2t_ref, gft,
           xt, aint, ahalo, idx, w0, w1t, gt, st, s, e1t, o1, r1, g0, h0, zpart, d1t, z0t, h1t, g1, zh, z1part, z1t,
           w0t, w1, gtp, ft, e0t, o0, r0, load_sem, halo_send, halo_recv, *sum_refs):
    dims = torus_dims(n)
    strides = tuple(dims[i + 1] * dims[i + 2] * dims[i + 3] if i == 0 else (dims[2] * dims[3], dims[3], 1)[i - 1] for i in range(4))
    me = lax.axis_index("nodes")
    pos = [lax.rem(lax.div(me, stride), d) for stride, d in zip(strides, dims)]
    feats, nodes = xt.shape
    classes, hidden = w1t.shape

    barrier = pltpu.get_barrier_semaphore()

    def greet(i):
        pl.semaphore_signal(barrier, inc=1, device_id={"nodes": lax.rem(me + i, n)})


    loads = [pltpu.make_async_copy(src, dst, load_sem.at[i]) for i, (src, dst) in enumerate([
        (idx_hbm, idx), (xt_hbm, xt), (w1t_hbm, w1t), (gt_hbm, gt), (aint_hbm, aint), (w0_hbm, w0)])]
    for load in loads[:4]:
        load.start()
    for c, k in enumerate(BLOCKS):
        pltpu.make_async_copy(
            ahalo_hbm.at[:, pl.ds(k * SLOTS, SLOTS)], ahalo.at[c // 2, :, pl.ds(c % 2 * SLOTS, SLOTS)], load_sem.at[6]).start()
    for load in loads[4:]:
        load.start()
    for i in (1, 2, n - 2, n - 1):
        greet(i)
    pl.loop(3, n - 2)(greet)

    ahead = lax.div(pos[2], dims[2] // 2)
    behind = 1 - ahead

    class Halo:
        def __init__(self, which, src, dst, sign):
            self.src, self.dst = src, dst
            self.send, self.recv = halo_send.at[which], [halo_recv.at[2 * which], halo_recv.at[2 * which + 1]]
            self.which, self.sign = which, sign
            self.first, self.second = (behind, ahead) if sign > 0 else (ahead, behind)

        def start(self):
            for c in ISSUE:
                o = OFFSETS[BLOCKS[c]]
                pltpu.make_async_remote_copy(
                    src_ref=self.src.at[c // 2, c % 2], dst_ref=self.dst.at[c // 2, c % 2], send_sem=self.send, recv_sem=self.recv[c // 2],
                    device_id={"nodes": lax.rem(me + self.sign * o + n, n)}).start()

        def wait_recv(self, half):
            wait_bytes(self.dst.at[half], halo_recv.at[2 * self.which + half])

        def wait_send(self):
            wait_bytes(self.src, self.send)

    halo_x = Halo(0, g0, h0, 1)
    halo_d1 = Halo(1, o1, r1, -1)
    halo_z = Halo(2, g1, zh, 1)
    halo_d0 = Halo(3, o0, r0, -1)
    sums = []
    for i, (_, _, _, stages) in enumerate(SUMS):
        refs = sum_refs[5 * i:5 * i + 5]
        sums.append(Sum(me, pos, dims, strides, stages, refs[0].shape[0], *refs))

    def put(ref, value):
        for c in range(4):
            ref[c // 2, c % 2] = value[:, c * SLOTS:(c + 1) * SLOTS].astype(BF)

    def take(ref, half):
        return jnp.concatenate([ref[half, 0], ref[half, 1]], axis=1)

    def outward(rows):
        return jnp.concatenate([dot(rows, ahalo[0]), dot(rows, ahalo[1])], axis=1)

    def half_rows(half):
        return s[pl.ds(pl.multiple_of(half * 2 * SLOTS, 2 * SLOTS), 2 * SLOTS)]

    loads[0].wait()
    sub = lax.broadcasted_iota(jnp.int32, (nodes, SLOTS), 0)
    for c, k in enumerate(BLOCKS):
        row = jnp.broadcast_to(idx[k:k + 1, :], (nodes, SLOTS))
        st[:, c * SLOTS:(c + 1) * SLOTS] = jnp.where(row == sub, 1.0, 0.0).astype(BF)

    loads[1].wait()
    put(g0, dot(xt[...], st[...]))
    loads[2].wait()
    loads[3].wait()
    w1[...] = jnp.concatenate([w1t[...].astype(F32), jnp.zeros((128 - classes, hidden), F32)], axis=0).T.astype(BF)
    gtp[...] = jnp.concatenate([gt[...].astype(F32), jnp.zeros((128 - classes, nodes), F32)], axis=0).astype(BF)
    e1t[...] = dot(w1[...], gtp[...]).astype(BF)
    wait_bytes(ahalo, load_sem.at[6])
    put(o1, outward(e1t[...]))

    pl.semaphore_wait(barrier, n - 1)
    halo_x.start()

    loads[4].wait()
    loads[5].wait()
    zpart[...] = dot_nt(xt[...], aint[...])
    halo_d1.start()
    w0t[...] = w0[...].astype(F32).T.astype(BF)
    lane = lax.broadcasted_iota(jnp.int32, (SLOTS, SLOTS), 1)
    for c, k in enumerate(BLOCKS):
        col = jnp.broadcast_to(idx[k:k + 1, :], (SLOTS, SLOTS)).T
        for b in range(nodes // SLOTS):
            s[c * SLOTS:(c + 1) * SLOTS, b * SLOTS:(b + 1) * SLOTS] = jnp.where(col == lane + b * SLOTS, 1.0, 0.0).astype(BF)
    d1t[...] = dot(e1t[...], aint[...])

    def hidden_of(zt):
        return jnp.maximum(dot(w0t[...], zt), 0.0).astype(BF)

    halo_x.wait_recv(halo_x.first)
    zpart[...] = zpart[...] + dot_nt(take(h0, halo_x.first), ahalo[halo_x.first])
    halo_x.wait_recv(halo_x.second)
    z0t[...] = (zpart[...] + dot_nt(take(h0, halo_x.second), ahalo[halo_x.second])).astype(BF)
    put(g1, dot(z0t[...], st[...]))
    halo_z.start()
    h1t[...] = hidden_of(z0t[...])
    z1part[...] = dot_nt(h1t[...], aint[...])

    halo_d1.wait_recv(halo_d1.first)
    d1t[...] = d1t[...] + dot(take(r1, halo_d1.first), half_rows(halo_d1.first))
    halo_d1.wait_recv(halo_d1.second)
    d1 = d1t[...] + dot(take(r1, halo_d1.second), half_rows(halo_d1.second))
    ft[...] = jnp.where(h1t[...] > 0, d1, 0.0).astype(BF)

    def to_chunks(which, value):
        groups = value.shape[0] // 8
        for (weight, lo, hi, _), total in zip(SUMS, sums):
            if weight == which:
                for k in range(lo, hi):
                    total.ar[(k - lo) * groups:(k - lo + 1) * groups] = value[:, k * 128:(k + 1) * 128].reshape(groups, 8, 128)

    def step(i):
        weight, lo, hi, _ = SUMS[i]
        if sums[i].step():
            return
        left.remove(i)
        out_ref, rows = (dw1_ref, feats) if weight == 1 else (dw2t_ref, classes)
        groups = sums[i].res.shape[0] // (hi - lo)
        for k in range(lo, hi):
            out_ref[:, k * 128:(k + 1) * 128] = sums[i].res[(k - lo) * groups:(k - lo + 1) * groups].reshape(groups * 8, 128)[0:rows]

    left = list(range(len(SUMS)))
    for event in ORDER:
        if event == "W":
            to_chunks(1, dot_nt(z0t[...], ft[...]))
        elif event == "E":
            e0t[...] = dot(w0[...], ft[...]).astype(BF)
            put(o0, outward(e0t[...]))
            halo_d0.start()
        elif event == "Z":
            halo_z.wait_recv(halo_z.first)
            z1part[...] = z1part[...] + dot_nt(hidden_of(take(zh, halo_z.first)), ahalo[halo_z.first])
            halo_z.wait_recv(halo_z.second)
            z1t[...] = (z1part[...] + dot_nt(hidden_of(take(zh, halo_z.second)), ahalo[halo_z.second])).astype(BF)
            padded = -(-classes // 8) * 8
            to_chunks(2, dot_nt(gtp[...], z1t[...])[0:padded])
        elif event == "g":
            gft[...] = dot(e0t[...], aint[...])
        elif event == "d":
            for half in range(2):
                halo_d0.wait_recv(half)
                gft[...] = gft[...] + dot(take(r0, half), half_rows(half))
        else:
            step("abcABC".index(event))
    assert not left
    for halo in (halo_x, halo_d1, halo_z, halo_d0):
        halo.wait_send()
    for total in sums:
        total.drain()


def write_out(a, b, c, x, y, z, sem):
    copies = [pltpu.make_async_copy(src, dst, sem.at[i]) for i, (src, dst) in enumerate([(a, x), (b, y), (c, z)])]
    for copy in copies:
        copy.start()
    for copy in copies:
        copy.wait()


def solution(mesh):
    n = mesh.shape["nodes"]
    dims = torus_dims(n)
    row_spec = P(("graph", "nodes"), None)
    replicated = P(None, None)
    part_spec = P("graph", None)

    def device_step(node_feats, a_int, a_halo, send_idx, w_first, w_second, grad_out):
        nodes, feats = node_feats.shape
        hidden, classes = w_second.shape
        slots = a_halo.shape[1]
        v = pltpu.VMEM
        dma = pltpu.SemaphoreType.DMA
        groups = {1: feats // 8, 2: -(-classes // 8)}
        sum_refs = []
        for weight, lo, hi, stages in SUMS:
            count = groups[weight] * (hi - lo)
            received = sum(p[5] for p in plan(dims, stages, count))
            sum_refs += [v((count, 8, 128), F32), v((count, 8, 128), F32), v((received, 8, 128), F32), dma((len(stages),)), dma((len(stages),))]
        outs = pl.pallas_call(
            functools.partial(kernel, n),
            out_shape=(v((feats, hidden), F32), v((classes, hidden), F32), v((feats, nodes), F32)),
            in_specs=[ANY] * 7,
            out_specs=[VMEM] * 3,
            scratch_shapes=[
                v((feats, nodes), BF),
                v((nodes, nodes), BF),
                v((2, nodes, slots // 2), BF),
                v((4, SLOTS), jnp.int32),
                v((feats, hidden), BF),
                v((classes, hidden), BF),
                v((classes, nodes), BF),
                v((nodes, slots), BF),
                v((slots, nodes), BF),
                v((hidden, nodes), BF),
                v((2, 2, hidden, SLOTS), BF),
                v((2, 2, hidden, SLOTS), BF),
                v((2, 2, feats, SLOTS), BF),
                v((2, 2, feats, SLOTS), BF),
                v((feats, nodes), F32),
                v((hidden, nodes), F32),
                v((feats, nodes), BF),
                v((hidden, nodes), BF),
                v((2, 2, feats, SLOTS), BF),
                v((2, 2, feats, SLOTS), BF),
                v((hidden, nodes), F32),
                v((hidden, nodes), BF),
                v((hidden, feats), BF),
                v((hidden, 128), BF),
                v((128, nodes), BF),
                v((hidden, nodes), BF),
                v((feats, nodes), BF),
                v((2, 2, feats, SLOTS), BF),
                v((2, 2, feats, SLOTS), BF),
                dma((7,)), dma((4,)), dma((8,)),
                *sum_refs,
            ],
            compiler_params=pltpu.CompilerParams(collective_id=0, has_side_effects=True, vmem_limit_bytes=40 << 20),
        )(*[pltpu.with_memory_space_constraint(a, pltpu.HBM) for a in
            (node_feats.T, a_int, a_halo, send_idx, w_first, w_second.T, grad_out.T)])
        dw1, dw2t, gft = pl.pallas_call(
            write_out,
            out_shape=tuple(jax.ShapeDtypeStruct(o.shape, F32) for o in outs),
            in_specs=[VMEM] * 3,
            out_specs=[ANY] * 3,
            scratch_shapes=[dma((3,))],
            compiler_params=pltpu.CompilerParams(vmem_limit_bytes=1 << 20),
        )(*outs)
        return dw1, dw2t.T, gft.T

    return jax.shard_map(device_step, mesh=mesh, in_specs=(row_spec, row_spec, row_spec, row_spec, replicated, replicated, row_spec), out_specs=(part_spec, part_spec, row_spec), check_vma=False)
```

```python
import functools

import jax
import jax.numpy as jnp
from jax import lax
from jax.experimental import pallas as pl
from jax.experimental.pallas import tpu as pltpu
from jax.sharding import PartitionSpec as P

BF = jnp.bfloat16
F32 = jnp.float32
OFFSETS = (1, -1, 2, -2)
BLOCKS = (0, 2, 1, 3)
ISSUE = (0, 2, 1, 3)
SLOTS = 128
ANY = pl.BlockSpec(memory_space=pl.ANY)
VMEM = pl.BlockSpec(memory_space=pltpu.VMEM)
FULL = (("rs", "c"), ("rs", "zyx"), ("ag", "zyx"), ("ag", "c"))
PLANE = (("rs", "zy"), ("bc", "xc"), ("ag", "zy"))
SUMS = (
    (1, 0, 4, FULL),
    (2, 0, 4, PLANE),
)
ORDER = "WaEZbabgabdaab"
AXES = "zyxc"


def torus_dims(n):
    return {128: (4, 4, 4, 2), 16: (2, 2, 2, 2)}[n]


def dot(a, b):
    return jnp.dot(a, b, preferred_element_type=F32)


def dot_nt(a, b):
    return lax.dot_general(a, b, (((1,), (1,)), ((), ())), preferred_element_type=F32)


def plan(dims, stages, count):
    out, stack = [], []
    for kind, axes in stages:
        size = 1
        for a in axes:
            size *= dims[AXES.index(a)]
        if kind == "rs":
            piece = next(p for p in range(-(-count // size), count + 1) if count % p == 0)
            owners = count // piece
            out.append((kind, axes, size, owners, piece, (size - 1) * piece))
            stack.append((count, owners))
            count = piece
        elif kind == "bc":
            out.append((kind, axes, size, size, count, size * count))
        else:
            whole, owners = stack.pop()
            out.append((kind, axes, size, owners, count, 0))
            count = whole
    return out


def wait_bytes(ref, sem):
    pltpu.make_async_copy(ref, ref, sem).wait()


def when(condition, body):
    if condition is None:
        body()
    else:
        pl.when(condition)(body)


def both(a, b):
    if a is None or b is None:
        return b if a is None else a
    return jnp.logical_and(a, b)


class Sum:
    def __init__(self, me, pos, dims, strides, stages, count, ar, res, rb, send_sem, recv_sem):
        self.me, self.pos, self.dims, self.strides = me, pos, dims, strides
        self.ar, self.res, self.rb, self.send_sem, self.recv_sem = ar, res, rb, send_sem, recv_sem
        self.plan = plan(dims, stages, count)
        self.drains = []
        self.steps = self.run(count)

    def group(self, axes):
        ids = [AXES.index(a) for a in axes]
        p, base = 0, self.me
        for a in ids:
            p = p * self.dims[a] + self.pos[a]
            base = base - self.pos[a] * self.strides[a]

        def device(q):
            out = base
            for a in reversed(ids):
                out = out + lax.rem(q, self.dims[a]) * self.strides[a]
                q = lax.div(q, self.dims[a])
            return out
        def partner(i):
            to, radix = 0, 1
            for a in reversed(ids):
                d = self.dims[a]
                to = to + lax.rem(self.pos[a] + lax.rem(i, d) + 1, d) * radix
                i, radix = lax.div(i, d), radix * d
            return to

        own = 0
        for a in ids:
            own = own * self.dims[a] + (self.dims[a] - 1)
        return p, device, partner, own

    def others(self, size, own, body):
        if size <= 8:
            for i in range(size):
                if i != own:
                    body(jnp.int32(i), i - (i > own))
            return

        @pl.loop(0, own)
        def _(i):
            body(i, i)

        @pl.loop(own + 1, size)
        def _(i):
            body(i, i - 1)

    def each(self, size, body, first=1):
        if size <= 8:
            for d in range(first, size):
                body(d)
        else:
            pl.loop(first, size)(body)

    def step(self):
        return next(self.steps, False)

    def run(self, count):
        ar, res, rb = self.ar, self.res, self.rb
        first, active, offset, stack = 0, None, 0, []
        for i, (kind, axes, size, owners, piece, slots) in enumerate(self.plan):
            p, device, partner, own = self.group(axes)
            send, recv = self.send_sem.at[i], self.recv_sem.at[i]
            to_of = lambda d: lax.rem(p + d, size)
            if kind == "rs":
                full = owners == size

                def start(i, slot):
                    to = partner(i)
                    copy = pltpu.make_async_remote_copy(
                        src_ref=ar.at[pl.ds(first + to * piece, piece)], dst_ref=rb.at[pl.ds(offset + slot * piece, piece)],
                        send_sem=send, recv_sem=recv, device_id={"nodes": device(to)})
                    when(None if full else to < owners, copy.start)
                when(active, lambda: self.others(size, own, start))
                yield True
                mine = both(active, None if full else p < owners)
                new = first + p * piece
                got = pl.ds(offset, slots)

                def collect():
                    wait_bytes(rb.at[got], recv)
                    total = ar[pl.ds(new, piece)] + jnp.sum(rb[got].reshape(size - 1, piece, 8, 128), axis=0)
                    ar[pl.ds(new, piece)] = total
                    res[pl.ds(new, piece)] = total
                when(mine, collect)
                if full:
                    self.drains.append((active, send, (size - 1) * piece))
                else:
                    self.drains.append((mine, send, (owners - 1) * piece))
                    self.drains.append((both(active, p >= owners), send, owners * piece))
                stack.append((first, active, p, full))
                first, active = new, mine
                offset += slots
            elif kind == "bc":
                mine = pl.ds(first, piece)

                def start(d):
                    to = to_of(d)
                    pltpu.make_async_remote_copy(
                        src_ref=ar.at[mine], dst_ref=rb.at[pl.ds(offset + p * piece, piece)],
                        send_sem=send, recv_sem=recv, device_id={"nodes": device(to)}).start()

                def spread():
                    self.each(size, start)
                    rb[pl.ds(offset + p * piece, piece)] = ar[mine]
                when(active, spread)
                yield True

                def collect():
                    wait_bytes(rb.at[pl.ds(offset, slots - piece)], recv)
                    res[mine] = jnp.sum(rb[pl.ds(offset, slots)].reshape(size, piece, 8, 128), axis=0)
                when(active, collect)
                self.drains.append((active, send, (size - 1) * piece))
                offset += slots
            else:
                mine = pl.ds(first, piece)
                ahead = axes == "zyx" and i + 1 < len(self.plan) and self.plan[i + 1][1] == "c"
                if axes == "c":
                    active = both(active, self.me >= 2)

                def start(to):
                    pl.when(to != p)(pltpu.make_async_remote_copy(
                        src_ref=res.at[mine], dst_ref=res.at[mine],
                        send_sem=send, recv_sem=recv, device_id={"nodes": device(to)}).start)

                def spread():
                    if ahead:
                        pltpu.make_async_remote_copy(
                            src_ref=res.at[mine], dst_ref=res.at[mine],
                            send_sem=send, recv_sem=self.recv_sem.at[i + 1], device_id={"nodes": 1 - self.pos[3]}).start()
                    self.each(size, start, 0)
                when(active, spread)
                yield True
                self.drains.append((active, send, (size - 1 + ahead) * piece))
                first, active, p, full = stack.pop()
                if full:
                    when(active, lambda: wait_bytes(res.at[pl.ds(0, (size - 1) * piece)], recv))
                else:
                    when(both(active, p < owners), lambda: wait_bytes(res.at[pl.ds(0, (owners - 1) * piece)], recv))
                    when(both(active, p >= owners), lambda: wait_bytes(res.at[pl.ds(0, owners * piece)], recv))

    def drain(self):
        for condition, sem, slots in self.drains:
            when(condition, lambda: wait_bytes(self.rb.at[pl.ds(0, slots)], sem))


def kernel(n, xt_hbm, aint_hbm, ahalo_hbm, idx_hbm, w0_hbm, w1t_hbm, gt_hbm, dw1_ref, dw2t_ref, gft,
           xt, aint, ahalo, idx, w0, w1t, gt, st, s, e1t, o1, r1, g0, h0, zpart, d1t, z0t, h1t, g1, zh, z1part, z1t,
           w0t, w1, gtp, ft, e0t, o0, r0, load_sem, halo_send, halo_recv, *sum_refs):
    dims = torus_dims(n)
    strides = tuple(dims[i + 1] * dims[i + 2] * dims[i + 3] if i == 0 else (dims[2] * dims[3], dims[3], 1)[i - 1] for i in range(4))
    me = lax.axis_index("nodes")
    pos = [lax.rem(lax.div(me, stride), d) for stride, d in zip(strides, dims)]
    feats, nodes = xt.shape
    classes, hidden = w1t.shape

    barrier = pltpu.get_barrier_semaphore()

    def greet(i):
        pl.semaphore_signal(barrier, inc=1, device_id={"nodes": lax.rem(me + i, n)})


    loads = [pltpu.make_async_copy(src, dst, load_sem.at[i]) for i, (src, dst) in enumerate([
        (idx_hbm, idx), (xt_hbm, xt), (w1t_hbm, w1t), (gt_hbm, gt), (aint_hbm, aint), (w0_hbm, w0)])]
    for load in loads[:4]:
        load.start()
    for c, k in enumerate(BLOCKS):
        pltpu.make_async_copy(
            ahalo_hbm.at[:, pl.ds(k * SLOTS, SLOTS)], ahalo.at[c // 2, :, pl.ds(c % 2 * SLOTS, SLOTS)], load_sem.at[6]).start()
    for load in loads[4:]:
        load.start()
    for i in (1, 2, n - 2, n - 1):
        greet(i)
    pl.loop(3, n - 2)(greet)

    ahead = lax.div(pos[2], dims[2] // 2)
    behind = 1 - ahead

    class Halo:
        def __init__(self, which, src, dst, sign):
            self.src, self.dst = src, dst
            self.send, self.recv = halo_send.at[which], [halo_recv.at[2 * which], halo_recv.at[2 * which + 1]]
            self.which, self.sign = which, sign
            self.first, self.second = (behind, ahead) if sign > 0 else (ahead, behind)

        def start(self):
            for c in ISSUE:
                o = OFFSETS[BLOCKS[c]]
                pltpu.make_async_remote_copy(
                    src_ref=self.src.at[c // 2, c % 2], dst_ref=self.dst.at[c // 2, c % 2], send_sem=self.send, recv_sem=self.recv[c // 2],
                    device_id={"nodes": lax.rem(me + self.sign * o + n, n)}).start()

        def wait_recv(self, half):
            wait_bytes(self.dst.at[half], halo_recv.at[2 * self.which + half])

        def wait_send(self):
            wait_bytes(self.src, self.send)

    halo_x = Halo(0, g0, h0, 1)
    halo_d1 = Halo(1, o1, r1, -1)
    halo_z = Halo(2, g1, zh, 1)
    halo_d0 = Halo(3, o0, r0, -1)
    sums = []
    for i, (_, _, _, stages) in enumerate(SUMS):
        refs = sum_refs[5 * i:5 * i + 5]
        sums.append(Sum(me, pos, dims, strides, stages, refs[0].shape[0], *refs))

    def put(ref, value):
        for c in range(4):
            ref[c // 2, c % 2] = value[:, c * SLOTS:(c + 1) * SLOTS].astype(BF)

    def take(ref, half):
        return jnp.concatenate([ref[half, 0], ref[half, 1]], axis=1)

    def outward(rows):
        return jnp.concatenate([dot(rows, ahalo[0]), dot(rows, ahalo[1])], axis=1)

    def half_rows(half):
        return s[pl.ds(pl.multiple_of(half * 2 * SLOTS, 2 * SLOTS), 2 * SLOTS)]

    loads[0].wait()
    sub = lax.broadcasted_iota(jnp.int32, (nodes, SLOTS), 0)
    for c, k in enumerate(BLOCKS):
        row = jnp.broadcast_to(idx[k:k + 1, :], (nodes, SLOTS))
        st[:, c * SLOTS:(c + 1) * SLOTS] = jnp.where(row == sub, 1.0, 0.0).astype(BF)

    loads[1].wait()
    put(g0, dot(xt[...], st[...]))
    loads[2].wait()
    loads[3].wait()
    w1[...] = jnp.concatenate([w1t[...].astype(F32), jnp.zeros((128 - classes, hidden), F32)], axis=0).T.astype(BF)
    gtp[...] = jnp.concatenate([gt[...].astype(F32), jnp.zeros((128 - classes, nodes), F32)], axis=0).astype(BF)
    e1t[...] = dot(w1[...], gtp[...]).astype(BF)
    wait_bytes(ahalo, load_sem.at[6])
    put(o1, outward(e1t[...]))

    pl.semaphore_wait(barrier, n - 1)
    halo_x.start()

    loads[4].wait()
    loads[5].wait()
    zpart[...] = dot_nt(xt[...], aint[...])
    halo_d1.start()
    w0t[...] = w0[...].astype(F32).T.astype(BF)
    lane = lax.broadcasted_iota(jnp.int32, (SLOTS, SLOTS), 1)
    for c, k in enumerate(BLOCKS):
        col = jnp.broadcast_to(idx[k:k + 1, :], (SLOTS, SLOTS)).T
        for b in range(nodes // SLOTS):
            s[c * SLOTS:(c + 1) * SLOTS, b * SLOTS:(b + 1) * SLOTS] = jnp.where(col == lane + b * SLOTS, 1.0, 0.0).astype(BF)
    d1t[...] = dot(e1t[...], aint[...])

    def hidden_of(zt):
        return jnp.maximum(dot(w0t[...], zt), 0.0).astype(BF)

    halo_x.wait_recv(halo_x.first)
    zpart[...] = zpart[...] + dot_nt(take(h0, halo_x.first), ahalo[halo_x.first])
    halo_x.wait_recv(halo_x.second)
    z0t[...] = (zpart[...] + dot_nt(take(h0, halo_x.second), ahalo[halo_x.second])).astype(BF)
    put(g1, dot(z0t[...], st[...]))
    halo_z.start()
    h1t[...] = hidden_of(z0t[...])
    z1part[...] = dot_nt(h1t[...], aint[...])

    halo_d1.wait_recv(halo_d1.first)
    d1t[...] = d1t[...] + dot(take(r1, halo_d1.first), half_rows(halo_d1.first))
    halo_d1.wait_recv(halo_d1.second)
    d1 = d1t[...] + dot(take(r1, halo_d1.second), half_rows(halo_d1.second))
    ft[...] = jnp.where(h1t[...] > 0, d1, 0.0).astype(BF)

    def to_chunks(which, value):
        groups = value.shape[0] // 8
        for (weight, lo, hi, _), total in zip(SUMS, sums):
            if weight == which:
                for k in range(lo, hi):
                    total.ar[(k - lo) * groups:(k - lo + 1) * groups] = value[:, k * 128:(k + 1) * 128].reshape(groups, 8, 128)

    def step(i):
        weight, lo, hi, _ = SUMS[i]
        if sums[i].step():
            return
        left.remove(i)
        out_ref, rows = (dw1_ref, feats) if weight == 1 else (dw2t_ref, classes)
        groups = sums[i].res.shape[0] // (hi - lo)
        for k in range(lo, hi):
            out_ref[:, k * 128:(k + 1) * 128] = sums[i].res[(k - lo) * groups:(k - lo + 1) * groups].reshape(groups * 8, 128)[0:rows]

    left = list(range(len(SUMS)))
    for event in ORDER:
        if event == "W":
            to_chunks(1, dot_nt(z0t[...], ft[...]))
        elif event == "E":
            e0t[...] = dot(w0[...], ft[...]).astype(BF)
            put(o0, outward(e0t[...]))
            halo_d0.start()
        elif event == "Z":
            halo_z.wait_recv(halo_z.first)
            z1part[...] = z1part[...] + dot_nt(hidden_of(take(zh, halo_z.first)), ahalo[halo_z.first])
            halo_z.wait_recv(halo_z.second)
            z1t[...] = (z1part[...] + dot_nt(hidden_of(take(zh, halo_z.second)), ahalo[halo_z.second])).astype(BF)
            padded = -(-classes // 8) * 8
            to_chunks(2, dot_nt(gtp[...], z1t[...])[0:padded])
        elif event == "g":
            gft[...] = dot(e0t[...], aint[...])
        elif event == "d":
            for half in range(2):
                halo_d0.wait_recv(half)
                gft[...] = gft[...] + dot(take(r0, half), half_rows(half))
        else:
            step("abcABC".index(event))
    assert not left
    for halo in (halo_x, halo_d1, halo_z, halo_d0):
        halo.wait_send()
    for total in sums:
        total.drain()


def write_out(a, b, c, x, y, z, sem):
    copies = [pltpu.make_async_copy(src, dst, sem.at[i]) for i, (src, dst) in enumerate([(a, x), (b, y), (c, z)])]
    for copy in copies:
        copy.start()
    for copy in copies:
        copy.wait()


def solution(mesh):
    n = mesh.shape["nodes"]
    dims = torus_dims(n)
    row_spec = P(("graph", "nodes"), None)
    replicated = P(None, None)
    part_spec = P("graph", None)

    def device_step(node_feats, a_int, a_halo, send_idx, w_first, w_second, grad_out):
        nodes, feats = node_feats.shape
        hidden, classes = w_second.shape
        slots = a_halo.shape[1]
        v = pltpu.VMEM
        dma = pltpu.SemaphoreType.DMA
        groups = {1: feats // 8, 2: -(-classes // 8)}
        sum_refs = []
        for weight, lo, hi, stages in SUMS:
            count = groups[weight] * (hi - lo)
            received = sum(p[5] for p in plan(dims, stages, count))
            sum_refs += [v((count, 8, 128), F32), v((count, 8, 128), F32), v((received, 8, 128), F32), dma((len(stages),)), dma((len(stages),))]
        outs = pl.pallas_call(
            functools.partial(kernel, n),
            out_shape=(v((feats, hidden), F32), v((classes, hidden), F32), v((feats, nodes), F32)),
            in_specs=[ANY] * 7,
            out_specs=[VMEM] * 3,
            scratch_shapes=[
                v((feats, nodes), BF),
                v((nodes, nodes), BF),
                v((2, nodes, slots // 2), BF),
                v((4, SLOTS), jnp.int32),
                v((feats, hidden), BF),
                v((classes, hidden), BF),
                v((classes, nodes), BF),
                v((nodes, slots), BF),
                v((slots, nodes), BF),
                v((hidden, nodes), BF),
                v((2, 2, hidden, SLOTS), BF),
                v((2, 2, hidden, SLOTS), BF),
                v((2, 2, feats, SLOTS), BF),
                v((2, 2, feats, SLOTS), BF),
                v((feats, nodes), F32),
                v((hidden, nodes), F32),
                v((feats, nodes), BF),
                v((hidden, nodes), BF),
                v((2, 2, feats, SLOTS), BF),
                v((2, 2, feats, SLOTS), BF),
                v((hidden, nodes), F32),
                v((hidden, nodes), BF),
                v((hidden, feats), BF),
                v((hidden, 128), BF),
                v((128, nodes), BF),
                v((hidden, nodes), BF),
                v((feats, nodes), BF),
                v((2, 2, feats, SLOTS), BF),
                v((2, 2, feats, SLOTS), BF),
                dma((7,)), dma((4,)), dma((8,)),
                *sum_refs,
            ],
            compiler_params=pltpu.CompilerParams(collective_id=0, has_side_effects=True, vmem_limit_bytes=40 << 20),
        )(*[pltpu.with_memory_space_constraint(a, pltpu.HBM) for a in
            (node_feats.T, a_int, a_halo, send_idx, w_first, w_second.T, grad_out.T)])
        dw1, dw2t, gft = pl.pallas_call(
            write_out,
            out_shape=tuple(jax.ShapeDtypeStruct(o.shape, F32) for o in outs),
            in_specs=[VMEM] * 3,
            out_specs=[ANY] * 3,
            scratch_shapes=[dma((3,))],
            compiler_params=pltpu.CompilerParams(vmem_limit_bytes=1 << 20),
        )(*outs)
        return dw1, dw2t.T, gft.T

    return jax.shard_map(device_step, mesh=mesh, in_specs=(row_spec, row_spec, row_spec, row_spec, replicated, replicated, row_spec), out_specs=(part_spec, part_spec, row_spec), check_vma=False)
```
